32 devices in a mesh: proto: 8 (over z, y), data: 4 (over x, core).
Axes of the slice: x: 2, y: 2, z: 4, core: 2. Of those that a mesh axis runs over, the one named last changes fastest.
Arguments:
- emb_one: bfloat16 [2048, 256], P('data')
- emb_two: bfloat16 [2048, 256], P('data')
- protos: bfloat16 [4096, 256], P('proto')
Outputs:
- output 1: float32 [2048, 4096], P('data', 'proto')
- output 2: float32 [2048, 4096], P('data', 'proto')
- output 3: float32 [], replicated
- output 4: float32 [2048, 256], P('data')
- output 5: float32 [2048, 256], P('data')
- output 6: float32 [4096, 256], P('proto')
All inputs are finite; a program needn't handle non-finite values.
Results may differ from the reference program's by a relative error of at most 0.001.
Values are sent between devices in bfloat16 or wider.
A program may use at most 1 GiB of HBM per device.

```python
import jax
import jax.numpy as jnp

ROWS_DEV = 512
DATA_GROUPS = 4
NUM_PROTOS = 4096
EMBED_DIM = 256
SINKHORN_ITERS = 3
EPSILON = 0.05
TEMP_TAU = 0.1
NOISE_SCALE = 0.8
TOTAL_ROWS = ROWS_DEV * DATA_GROUPS


def unit_rows(matrix):
    return matrix / jnp.sqrt(jnp.sum(matrix * matrix, axis=1, keepdims=True))


def setup_inputs(seed: int = 0) -> dict:
    key = jax.random.key(seed)
    key_protos, key_home, key_one, key_two = jax.random.split(key, 4)
    protos = unit_rows(jax.random.normal(key_protos, (NUM_PROTOS, EMBED_DIM), jnp.float32))
    shard_ids = jnp.arange(TOTAL_ROWS, dtype=jnp.int32) // ROWS_DEV
    home_ids = shard_ids + DATA_GROUPS * jax.random.randint(key_home, (TOTAL_ROWS,), 0, NUM_PROTOS // DATA_GROUPS)
    centers = protos[home_ids]
    noise_one = jax.random.normal(key_one, (TOTAL_ROWS, EMBED_DIM), jnp.float32) * (NOISE_SCALE * EMBED_DIM ** -0.5)
    noise_two = jax.random.normal(key_two, (TOTAL_ROWS, EMBED_DIM), jnp.float32) * (NOISE_SCALE * EMBED_DIM ** -0.5)
    return {'emb_one': unit_rows(centers + noise_one).astype(jnp.bfloat16),
            'emb_two': unit_rows(centers + noise_two).astype(jnp.bfloat16),
            'protos': protos.astype(jnp.bfloat16)}


def sinkhorn_codes(scores):
    transport = jnp.exp(scores / EPSILON)
    for _ in range(SINKHORN_ITERS):
        col_sum = jnp.sum(transport, axis=0)
        transport = transport / (NUM_PROTOS * col_sum)
        row_sum = jnp.sum(transport, axis=1, keepdims=True)
        transport = transport / (TOTAL_ROWS * row_sum)
    return TOTAL_ROWS * transport


def log_probs(scores):
    logits = scores / TEMP_TAU
    return logits - jnp.log(jnp.sum(jnp.exp(logits), axis=1, keepdims=True))


def reference(emb_one, emb_two, protos):
    scores_one = jnp.dot(emb_one, protos.T, preferred_element_type=jnp.float32)
    scores_two = jnp.dot(emb_two, protos.T, preferred_element_type=jnp.float32)
    codes_one = sinkhorn_codes(scores_one)
    codes_two = sinkhorn_codes(scores_two)
    logp_one = log_probs(scores_one)
    logp_two = log_probs(scores_two)
    loss_value = -(jnp.sum(codes_two * logp_one) + jnp.sum(codes_one * logp_two)) / (2 * TOTAL_ROWS)
    grad_scale = 2 * TOTAL_ROWS * TEMP_TAU
    logit_grad_one = ((jnp.exp(logp_one) - codes_two) / grad_scale).astype(jnp.bfloat16)
    logit_grad_two = ((jnp.exp(logp_two) - codes_one) / grad_scale).astype(jnp.bfloat16)
    grad_one = jnp.dot(logit_grad_one, protos, preferred_element_type=jnp.float32)
    grad_two = jnp.dot(logit_grad_two, protos, preferred_element_type=jnp.float32)
    grad_protos = (jnp.dot(logit_grad_one.T, emb_one, preferred_element_type=jnp.float32)
                   + jnp.dot(logit_grad_two.T, emb_two, preferred_element_type=jnp.float32))
    return codes_one, codes_two, loss_value, grad_one, grad_two, grad_protos
```

```python
import functools
import math

import jax
import jax.numpy as jnp
from jax import lax
from jax.experimental import pallas as pl
from jax.experimental.pallas import tpu as pltpu
from jax.sharding import PartitionSpec as P

TEMP_TAU = 0.1
ITERS = 3
F32, BF16 = jnp.float32, jnp.bfloat16
LOG2E_TAU = math.log2(math.e) / TEMP_TAU
LN2 = math.log(2.0)
B = 512
L = 128
CH = 64
NT = (((1,), (1,)), ((), ()))


def eye_mask():
    return lax.broadcasted_iota(jnp.int32, (L, L), 0) == lax.broadcasted_iota(jnp.int32, (L, L), 1)


def col_to_row(eye, col):
    return jnp.sum(jnp.where(eye, col, 0.0), axis=0, keepdims=True)


def row_to_col(eye, row):
    return jnp.sum(jnp.where(eye, row, 0.0), axis=1, keepdims=True)


def sinkhorn_kernel(np_, nd, z1, z2, c, zall, call, rowv, vvec,
                    T, A, vrep, ctx, crx, rtx, rrx, utx,
                    lsem, cs, cr, rs, rr, vs, vr, us, ur, zs, zr, gs, gr):
    p = lax.axis_index('proto')
    d = lax.axis_index('data')
    total_rows = nd * B
    total_protos = np_ * B
    core = lax.rem(d, 2)

    loads = [pltpu.make_async_copy(z1, zall.at[0, d], lsem.at[0]),
             pltpu.make_async_copy(z2, zall.at[1, d], lsem.at[1]),
             pltpu.make_async_copy(c, call.at[p], lsem.at[2])]
    for cp in loads:
        cp.start()

    def xor(a, k):
        out = a
        for bit in (1, 2, 4):
            if k & bit:
                has = lax.rem(out // bit, 2)
                out = out + bit - 2 * bit * has
        return out

    dpeers = [xor(d, j) for j in range(nd)]
    ppeers = [xor(p, j) for j in range(np_)]

    bar = pltpu.get_barrier_semaphore()
    for j in range(1, nd):
        pl.semaphore_signal(bar, inc=1, device_id={'proto': p, 'data': dpeers[j]})
    for j in range(1, np_):
        pl.semaphore_signal(bar, inc=1, device_id={'proto': ppeers[j], 'data': d})

    for cp in loads:
        cp.wait()

    def remote(src, dst, ss, rs_, pj, dj):
        return pltpu.make_async_remote_copy(src, dst, ss, rs_, device_id={'proto': ppeers[pj], 'data': dpeers[dj]})

    pend = []

    ZQ = B // 4
    HB = B // 2

    def z_piece(i):
        out = []
        for v in range(2):
            ref = zall.at[v, d, pl.ds(i * ZQ, ZQ)]
            cp = remote(ref, ref, zs.at[0, v, i], zr.at[0, v, i], 0, 2)
            cp.start()
            out.append(cp)
        pend.extend(out)
        return out

    def z_partner(src_d, slot):
        out = []
        for v in range(2):
            ref = zall.at[v, src_d]
            cp = remote(ref, ref, zs.at[slot, v, 0], zr.at[slot, v, 0], 0, 1)
            cp.start()
            out.append(cp)
        pend.extend(out)
        return out

    mine = pl.ds(pl.multiple_of(core * HB, HB), HB)

    def c_send(blk, slot, pj, dj):
        ref = call.at[blk, mine]
        cp = remote(ref, ref, gs.at[slot], gr.at[slot], pj, dj)
        cp.start()
        pend.append(cp)
        return cp

    eye = eye_mask()

    for v in range(2):
        T[v] = lax.dot_general(call[p], zall[v, d], NT, preferred_element_type=F32) * LOG2E_TAU
    crow = [None] * 8
    dsum = [None] * 8
    for v in range(2):
        dacc = [jnp.zeros((8, L), F32) for _ in range(4)]
        cols = []
        for ck in range(B // CH):
            rows = pl.ds(ck * CH, CH)
            part = None
            for j in range(4):
                e = jnp.exp2(T[v, rows, j * L:(j + 1) * L])
                a = e * e
                A[v, rows, j * L:(j + 1) * L] = a
                dacc[j] = dacc[j] + jnp.sum(e.reshape(CH // 8, 8, L), axis=0)
                part = a if part is None else part + a
            cols.append(jnp.sum(part, axis=1, keepdims=True))
        per = L // CH
        for i in range(4):
            crow[4 * v + i] = col_to_row(eye, jnp.concatenate(cols[per * i:per * (i + 1)], axis=0))
            dsum[4 * v + i] = jnp.sum(dacc[i], axis=0, keepdims=True)

    pl.semaphore_wait(bar, nd - 1 + np_ - 1)

    z_recv = []
    u_tile = None
    dfull = None
    for it in range(ITERS):
        for i in range(8):
            ctx[it, i:i + 1] = crow[i]
        cps = []
        for j in range(1, nd):
            cp = remote(ctx.at[it], crx.at[it, j], cs.at[it, j], cr.at[it, j], 0, j)
            cp.start()
            cps.append(cp)
        pend.extend(cps)
        if it == 0:
            zp1 = z_partner(d, 1)
            z_recv += z_piece(0)
            g_y = c_send(p, 0, 1, 0)
            g_z1 = c_send(p, 1, 2, 0)
        elif it == 1:
            z_recv += z_piece(2)
        ctot = ctx[it]
        for j, cp in zip(range(1, nd), cps):
            cp.wait_recv()
            ctot = ctot + crx[it, j]
        vt = 1.0 / (total_protos * ctot)
        if it == ITERS - 1:
            vvec[p] = vt
            vcps = []
            for j in range(1, np_):
                cp = remote(vvec.at[p], vvec.at[p], vs.at[j], vr.at[j], j, 0)
                cp.start()
                vcps.append(cp)
            pend.extend(vcps)
        for v in range(2):
            for i in range(4):
                vrep[v, i * L:(i + 1) * L] = jnp.broadcast_to(row_to_col(eye, vt[4 * v + i:4 * v + i + 1]), (L, L))
        last = it == ITERS - 1
        for v in range(2):
            racc = [jnp.zeros((8, L), F32) for _ in range(4)]
            tacc = [jnp.zeros((8, L), F32) for _ in range(4)]
            for ck in range(B // CH):
                rows = pl.ds(ck * CH, CH)
                w = vrep[v, rows]
                for j in range(4):
                    lanes = slice(j * L, (j + 1) * L)
                    m = A[v, rows, lanes] * w
                    racc[j] = racc[j] + jnp.sum(m.reshape(CH // 8, 8, L), axis=0)
                    if last:
                        mt = m * T[1 - v, rows, lanes]
                        tacc[j] = tacc[j] + jnp.sum(mt.reshape(CH // 8, 8, L), axis=0)
            for j in range(4):
                rtx[it, 4 * v + j:4 * v + j + 1] = jnp.sum(racc[j], axis=0, keepdims=True)
                if last:
                    rtx[it, 8 + 4 * v + j:8 + 4 * v + j + 1] = jnp.sum(tacc[j], axis=0, keepdims=True)
        if it == 0:
            for i in range(8):
                rtx[it, 8 + i:9 + i] = dsum[i]
        nrow = 8 if it == 1 else 16
        cps = []
        for j in range(1, np_):
            cp = remote(rtx.at[it, 0:nrow], rrx.at[it, j, 0:nrow], rs.at[it, j], rr.at[it, j], j, 0)
            cp.start()
            cps.append(cp)
        pend.extend(cps)
        if it == 0:
            z_recv += z_piece(1)
            g_y.wait_recv()
            g_z1.wait_recv()
            g_z2 = c_send(p, 2, 4, 0)
            g_y1 = c_send(ppeers[2], 3, 1, 0)
        elif it == 1:
            z_recv += z_piece(3)
            g_z2.wait_recv()
            g_z3 = c_send(p, 4, 6, 0)
            g_y2 = c_send(ppeers[4], 5, 1, 0)
        else:
            g_z3.wait_recv()
            g_y3 = c_send(ppeers[6], 6, 1, 0)
            for cp in z_recv:
                cp.wait_recv()
            zp2 = z_partner(dpeers[2], 2)
        rtot = rtx[it, 0:nrow]
        for j, cp in zip(range(1, np_), cps):
            cp.wait_recv()
            rtot = rtot + rrx[it, j, 0:nrow]
        if it == 0:
            dfull = rtot[8:16]
        u_tile = 1.0 / (total_rows * rtot[0:8])
        if not last:
            for v in range(2):
                cols = []
                for ck in range(B // CH):
                    rows = pl.ds(ck * CH, CH)
                    part = None
                    for j in range(4):
                        m = A[v, rows, j * L:(j + 1) * L] * u_tile[4 * v + j:4 * v + j + 1]
                        part = m if part is None else part + m
                    cols.append(jnp.sum(part, axis=1, keepdims=True))
                per = L // CH
                for i in range(4):
                    crow[4 * v + i] = col_to_row(eye, jnp.concatenate(cols[per * i:per * (i + 1)], axis=0))
    g_y1.wait_recv()
    g_y2.wait_recv()
    g_y3.wait_recv()
    gp = [c_send(k, 8 + k, 0, 1) for k in range(np_)]

    w = total_rows * u_tile
    logd = jnp.log(dfull)
    swapped = jnp.concatenate([logd[4:8], logd[0:4]], axis=0)
    terms = w * rtot[8:16] * LN2 - (w * rtot[0:8]) * swapped
    tot = jnp.sum(jnp.sum(terms, axis=1, keepdims=True), axis=0, keepdims=True)
    rowv[d, 0:8] = w
    rowv[d, 8:16] = 1.0 / dfull
    rowv[d, 16:24] = jnp.broadcast_to(tot, (8, L))
    ucps = []
    for j in range(1, nd):
        cp = remote(rowv.at[d], rowv.at[d], us.at[j], ur.at[j], 0, j)
        cp.start()
        ucps.append(cp)
    pend.extend(ucps)
    for cp in zp1 + zp2 + gp + ucps + vcps:
        cp.wait_recv()
    for cp in pend:
        cp.wait_send()


def grads_kernel(np_, nd, z1, z2, zall, call, rowv, vvec, q1, q2, loss, g1, g2, gp,
                 T, H, ucol, qbuf, sem):
    p = lax.axis_index('proto')
    d = lax.axis_index('data')
    total_rows = nd * B
    inv_scale = 1.0 / (2 * total_rows * TEMP_TAU)
    eye = eye_mask()
    lsum = rowv[0, 16:17, 0:1]
    for k in range(1, nd):
        lsum = lsum + rowv[k, 16:17, 0:1]
    loss[...] = lsum * (-1.0 / (2 * total_rows))

    for i in range(16):
        ucol[i // 4, (i % 4) * L:(i % 4 + 1) * L] = jnp.broadcast_to(
            row_to_col(eye, rowv[d, i:i + 1]) * inv_scale, (L, L))
    g1[...] = jnp.zeros_like(g1)
    g2[...] = jnp.zeros_like(g2)
    gp[...] = jnp.zeros_like(gp)
    za, zb = zall.at[0, d], zall.at[1, d]

    def scores(k, lhs_rows):
        cb = call[k]
        T[0] = lax.dot_general(za[...], cb, NT, preferred_element_type=F32) * LOG2E_TAU
        T[1] = lax.dot_general(zb[...], cb, NT, preferred_element_type=F32) * LOG2E_TAU

    def block(k, codes):
        scores(k, None)
        vt = vvec[k]
        for ck in range(B // CH):
            rows = pl.ds(ck * CH, CH)
            for j in range(4):
                lanes = slice(j * L, (j + 1) * L)
                e1 = jnp.exp2(T[0, rows, lanes])
                e2 = jnp.exp2(T[1, rows, lanes])
                a1 = (e1 * e1) * vt[j:j + 1] * ucol[0, rows]
                a2 = (e2 * e2) * vt[4 + j:5 + j] * ucol[1, rows]
                H[0, rows, lanes] = (e1 * ucol[2, rows] - a2).astype(BF16)
                H[1, rows, lanes] = (e2 * ucol[3, rows] - a1).astype(BF16)
                if codes:
                    qbuf[0, rows, lanes] = a1 * (1.0 / inv_scale)
                    qbuf[1, rows, lanes] = a2 * (1.0 / inv_scale)
        cb = call[k]
        g1[...] += jnp.dot(H[0], cb, preferred_element_type=F32)
        g2[...] += jnp.dot(H[1], cb, preferred_element_type=F32)

    block(p, True)
    out = [pltpu.make_async_copy(qbuf.at[0], q1, sem.at[0]), pltpu.make_async_copy(qbuf.at[1], q2, sem.at[1])]
    for cp in out:
        cp.start()

    def step(i, carry):
        block(lax.rem(p + i, np_), False)
        return carry

    lax.fori_loop(1, np_, step, 0)

    vt = vvec[p]
    for v in range(2):
        for i in range(4):
            ucol[v, i * L:(i + 1) * L] = jnp.broadcast_to(row_to_col(eye, vt[4 * v + i:4 * v + i + 1]), (L, L))
    cown = call.at[p]

    def cstep(k, carry):
        zk1, zk2 = zall[0, k], zall[1, k]
        T[0] = lax.dot_general(cown[...], zk1, NT, preferred_element_type=F32) * LOG2E_TAU
        T[1] = lax.dot_general(cown[...], zk2, NT, preferred_element_type=F32) * LOG2E_TAU
        rv = rowv[k, 0:16] * inv_scale
        for ck in range(B // CH):
            rows = pl.ds(ck * CH, CH)
            for j in range(4):
                lanes = slice(j * L, (j + 1) * L)
                e1 = jnp.exp2(T[0, rows, lanes])
                e2 = jnp.exp2(T[1, rows, lanes])
                a1 = (e1 * e1) * rv[j:j + 1] * ucol[0, rows]
                a2 = (e2 * e2) * rv[4 + j:5 + j] * ucol[1, rows]
                H[0, rows, lanes] = (e1 * rv[8 + j:9 + j] - a2).astype(BF16)
                H[1, rows, lanes] = (e2 * rv[12 + j:13 + j] - a1).astype(BF16)
        gp[...] += jnp.dot(H[0], zk1, preferred_element_type=F32) + jnp.dot(H[1], zk2, preferred_element_type=F32)
        return carry

    lax.fori_loop(0, nd, cstep, 0)
    for cp in out:
        cp.wait()


def solution(mesh):
    np_ = mesh.shape['proto']
    nd = mesh.shape['data']
    VM = pl.BlockSpec(memory_space=pltpu.VMEM)
    ANY = pl.BlockSpec(memory_space=pl.ANY)
    DMA = pltpu.SemaphoreType.DMA

    def local_step(emb_one, emb_two, protos):
        dim = protos.shape[1]
        zall, call, rowv, vvec = pl.pallas_call(
            functools.partial(sinkhorn_kernel, np_, nd),
            out_shape=(jax.ShapeDtypeStruct((2, nd, B, dim), BF16), jax.ShapeDtypeStruct((np_, B, dim), BF16),
                       jax.ShapeDtypeStruct((nd, 24, L), F32), jax.ShapeDtypeStruct((np_, 8, L), F32)),
            in_specs=[ANY] * 3, out_specs=(VM,) * 4,
            scratch_shapes=[
                pltpu.VMEM((2, B, B), F32), pltpu.VMEM((2, B, B), F32), pltpu.VMEM((2, B, L), F32),
                pltpu.VMEM((ITERS, 8, L), F32), pltpu.VMEM((ITERS, nd, 8, L), F32),
                pltpu.VMEM((ITERS, 16, L), F32), pltpu.VMEM((ITERS, np_, 16, L), F32), pltpu.VMEM((8, L), F32),
                DMA((3,)), DMA((ITERS, nd)), DMA((ITERS, nd)), DMA((ITERS, np_)), DMA((ITERS, np_)),
                DMA((np_,)), DMA((np_,)), DMA((nd,)), DMA((nd,)),
                DMA((3, 2, 4)), DMA((3, 2, 4)), DMA((16,)), DMA((16,))],
            compiler_params=pltpu.CompilerParams(collective_id=0, has_side_effects=True),
            name='sinkhorn',
        )(emb_one, emb_two, protos)
        q1, q2, loss, g1, g2, gp = pl.pallas_call(
            functools.partial(grads_kernel, np_, nd),
            out_shape=(jax.ShapeDtypeStruct((B, B), F32), jax.ShapeDtypeStruct((B, B), F32),
                       jax.ShapeDtypeStruct((1, 1), F32),
                       jax.ShapeDtypeStruct((B, dim), F32), jax.ShapeDtypeStruct((B, dim), F32),
                       jax.ShapeDtypeStruct((B, dim), F32)),
            in_specs=[ANY, ANY] + [VM] * 4, out_specs=(ANY, ANY, VM, VM, VM, VM),
            scratch_shapes=[pltpu.VMEM((2, B, B), F32), pltpu.VMEM((2, B, B), BF16), pltpu.VMEM((4, B, L), F32),
                            pltpu.VMEM((2, B, B), F32), DMA((2,))],
            name='grads',
        )(emb_one, emb_two, zall, call, rowv, vvec)
        return q1, q2, loss.reshape(()), g1, g2, gp

    return jax.shard_map(
        local_step, mesh=mesh,
        in_specs=(P('data', None), P('data', None), P('proto', None)),
        out_specs=(P('data', 'proto'), P('data', 'proto'), P(), P('data', None), P('data', None), P('proto', None)),
        check_vma=False)
```

```python
import functools
import math

import jax
import jax.numpy as jnp
from jax import lax
from jax.experimental import pallas as pl
from jax.experimental.pallas import tpu as pltpu
from jax.sharding import PartitionSpec as P

TEMP_TAU = 0.1
ITERS = 3
F32, BF16 = jnp.float32, jnp.bfloat16
LOG2E_TAU = math.log2(math.e) / TEMP_TAU
LN2 = math.log(2.0)
B = 512
HB = 256
L = 128
CH = 64
NT = (((1,), (1,)), ((), ()))


def eye_mask():
    return lax.broadcasted_iota(jnp.int32, (L, L), 0) == lax.broadcasted_iota(jnp.int32, (L, L), 1)


def col_to_row(eye, col):
    return jnp.sum(jnp.where(eye, col, 0.0), axis=0, keepdims=True)


def row_to_col(eye, row):
    return jnp.sum(jnp.where(eye, row, 0.0), axis=1, keepdims=True)


def xor(a, k):
    out = a
    for bit in (1, 2, 4):
        if k & bit:
            out = out + bit - 2 * bit * lax.rem(out // bit, 2)
    return out


def sinkhorn_kernel(np_, nd, z1, z2, c, zall, call, E, ET, rowv, vvec, vrep,
                    T, A, ctx, crx, rtx, rrx,
                    lsem, cs, cr, rs, rr, vs, vr, us, ur, zs, zr, gs, gr, ds_, dr_):
    p = lax.axis_index('proto')
    d = lax.axis_index('data')
    total_rows = nd * B
    total_protos = np_ * B
    core = lax.rem(d, 2)
    half = core
    other = 1 - core

    loads = [pltpu.make_async_copy(z1.at[h * HB:(h + 1) * HB], zall.at[0, 2 * d + h], lsem.at[h]) for h in range(2)]
    loads += [pltpu.make_async_copy(z2.at[h * HB:(h + 1) * HB], zall.at[1, 2 * d + h], lsem.at[2 + h]) for h in range(2)]
    loads += [pltpu.make_async_copy(c.at[h * HB:(h + 1) * HB], call.at[2 * p + h], lsem.at[4 + h]) for h in range(2)]
    for cp in loads:
        cp.start()

    dp = [xor(d, j) for j in range(nd)]
    pp = [xor(p, j) for j in range(np_)]

    bar = pltpu.get_barrier_semaphore()
    for j in range(1, nd):
        pl.semaphore_signal(bar, inc=1, device_id={'proto': p, 'data': dp[j]})
    for j in range(1, np_):
        pl.semaphore_signal(bar, inc=1, device_id={'proto': pp[j], 'data': d})

    for cp in loads:
        cp.wait()

    pend = []

    def send(src, dst, ss, rs_, pj, dj):
        cp = pltpu.make_async_remote_copy(src, dst, ss, rs_, device_id={'proto': pp[pj], 'data': dp[dj]})
        cp.start()
        pend.append(cp)
        return cp

    def z_x(i):
        ref = zall.at[i // 2, 2 * d + i % 2]
        return send(ref, ref, zs.at[i], zr.at[i], 0, 2)

    def z_partner(slot, v, nb):
        ref = zall.at[v, nb]
        return send(ref, ref, zs.at[slot], zr.at[slot], 0, 1)

    def c_send(slot, q, pj, rows=None):
        ref = call.at[2 * q + half] if rows is None else call.at[2 * q + half, rows]
        return send(ref, ref, gs.at[slot], gr.at[slot], pj, 0)

    def c_partner(j):
        ref = call.at[2 * pp[j] + half]
        return send(ref, ref, ds_.at[j], dr_.at[j], 0, 1)

    def scores_rows(hb):
        def body(v, carry):
            zz = zall[v, pl.ds(2 * d, 2)].reshape(B, -1)
            s = lax.dot_general(zz, call[hb], NT, preferred_element_type=F32)
            E[v, hb] = jnp.exp2(s * LOG2E_TAU)
            return carry
        for v in range(2):
            body(v, 0)

    def scores_cols(nb):
        def body(v, carry):
            cc = call[pl.ds(2 * p, 2)].reshape(B, -1)
            s = lax.dot_general(cc, zall[v, nb], NT, preferred_element_type=F32)
            ET[v, nb] = jnp.exp2(s * LOG2E_TAU)
            return carry
        for v in range(2):
            body(v, 0)

    eye = eye_mask()

    crow = [None] * 8
    dsum = [None] * 8
    for v in range(2):
        for h in range(2):
            for h2 in range(2):
                T[v, h * HB:(h + 1) * HB, h2 * HB:(h2 + 1) * HB] = lax.dot_general(
                    call[2 * p + h], zall[v, 2 * d + h2], NT, preferred_element_type=F32) * LOG2E_TAU

    per = L // CH

    def finish_cols(v, cols):
        for i in range(4):
            crow[4 * v + i] = col_to_row(eye, jnp.concatenate(cols[per * i:per * (i + 1)], axis=0))

    for v in range(2):
        dacc = [jnp.zeros((8, L), F32) for _ in range(4)]
        cols = []
        for ck in range(B // CH):
            rows = pl.ds(ck * CH, CH)
            part = None
            for j in range(4):
                e = jnp.exp2(T[v, rows, j * L:(j + 1) * L])
                a = e * e
                ET[v, 2 * d + j // 2, rows, (j % 2) * L:(j % 2 + 1) * L] = e
                A[v, rows, j * L:(j + 1) * L] = a
                dacc[j] = dacc[j] + jnp.sum(e.reshape(CH // 8, 8, L), axis=0)
                part = a if part is None else part + a
            cols.append(jnp.sum(part, axis=1, keepdims=True))
        finish_cols(v, cols)
        for j in range(4):
            dsum[4 * v + j] = jnp.sum(dacc[j], axis=0, keepdims=True)

    pl.semaphore_wait(bar, nd - 1 + np_ - 1)

    bulk = {}
    QR = [pl.ds(0, L), pl.ds(L, L)]

    def background(it, along_data):
        if it == 0 and along_data:
            for v in range(2):
                for h in range(2):
                    bulk['zp', v, h] = z_partner(4 + 2 * v + h, v, 2 * d + h)
            bulk['zx', 0] = z_x(0)
            bulk['y0'] = c_send(0, p, 1)
            bulk['z2'] = c_send(1, p, 2)
            bulk['z4a'] = c_send(2, p, 4, QR[0])
            scores_rows(2 * p)
            scores_rows(2 * p + 1)
        elif it == 0:
            bulk['zx', 1] = z_x(1)
            bulk['z4b'] = c_send(3, p, 4, QR[1])
            for v in range(2):
                for h in range(2):
                    bulk['zp', v, h].wait_recv()
            scores_cols(2 * dp[1])
            scores_cols(2 * dp[1] + 1)
            bulk['y0'].wait_recv()
            bulk['d1'] = c_partner(1)
            bulk['z2'].wait_recv()
            bulk['d2'] = c_partner(2)
            bulk['y2'] = c_send(6, pp[2], 1)
        elif it == 1 and along_data:
            bulk['zx', 2] = z_x(2)
            bulk['z6a'] = c_send(4, p, 6, QR[0])
            scores_rows(2 * pp[1] + half)
            scores_rows(2 * pp[2] + half)
        elif it == 1:
            bulk['zx', 3] = z_x(3)
            bulk['z6b'] = c_send(5, p, 6, QR[1])
            bulk['z4a'].wait_recv()
            bulk['z4b'].wait_recv()
            bulk['d4'] = c_partner(4)
            bulk['y4'] = c_send(7, pp[4], 1)
            bulk['d1'].wait_recv()
            scores_rows(2 * pp[1] + other)
            bulk['d2'].wait_recv()
            scores_rows(2 * pp[2] + other)
            bulk['y2'].wait_recv()
            bulk['d3'] = c_partner(3)
            scores_rows(2 * pp[4] + half)
        elif it == 2 and along_data:
            bulk['z6a'].wait_recv()
            bulk['z6b'].wait_recv()
            bulk['d6'] = c_partner(6)
            bulk['y6'] = c_send(8, pp[6], 1)
            for i in range(4):
                bulk['zx', i].wait_recv()
                bulk['zf', i] = z_partner(8 + i, i // 2, 2 * dp[2] + i % 2)
            scores_rows(2 * pp[3] + half)
            scores_rows(2 * pp[6] + half)
        elif it == 2:
            bulk['y4'].wait_recv()
            bulk['d5'] = c_partner(5)
            scores_cols(2 * dp[2])
            scores_cols(2 * dp[2] + 1)
            for j in (3, 4):
                bulk['d%d' % j].wait_recv()
                scores_rows(2 * pp[j] + other)
            bulk['y6'].wait_recv()
            bulk['d7'] = c_partner(7)
            scores_rows(2 * pp[5] + half)
            scores_rows(2 * pp[7] + half)
        else:
            for i in range(4):
                bulk['zf', i].wait_recv()
            scores_cols(2 * dp[3])
            scores_cols(2 * dp[3] + 1)
            for j in (6, 5, 7):
                bulk['d%d' % j].wait_recv()
                scores_rows(2 * pp[j] + other)

    for it in range(ITERS):
        last = it == ITERS - 1
        for i in range(8):
            ctx[it, i:i + 1] = crow[i]
        cps = [send(ctx.at[it], crx.at[it, j], cs.at[it, j], cr.at[it, j], 0, j) for j in range(1, nd)]
        background(it, True)
        ctot = ctx[it]
        for j, cp in zip(range(1, nd), cps):
            cp.wait_recv()
            ctot = ctot + crx[it, j]
        vt = 1.0 / (total_protos * ctot)
        if last:
            vvec[p] = vt
            vcps = [send(vvec.at[p], vvec.at[p], vs.at[j], vr.at[j], j, 0) for j in range(1, np_)]
        for v in range(2):
            for i in range(4):
                vrep[v, i * L:(i + 1) * L] = jnp.broadcast_to(row_to_col(eye, vt[4 * v + i:4 * v + i + 1]), (L, L))
        for v in range(2):
            racc = [jnp.zeros((8, L), F32) for _ in range(4)]
            tacc = [jnp.zeros((8, L), F32) for _ in range(4)]
            for ck in range(B // CH):
                rows = pl.ds(ck * CH, CH)
                w = vrep[v, rows]
                for j in range(4):
                    lanes = slice(j * L, (j + 1) * L)
                    m = A[v, rows, lanes] * w
                    racc[j] = racc[j] + jnp.sum(m.reshape(CH // 8, 8, L), axis=0)
                    if last:
                        mt = m * T[1 - v, rows, lanes]
                        tacc[j] = tacc[j] + jnp.sum(mt.reshape(CH // 8, 8, L), axis=0)
            for j in range(4):
                rtx[it, 4 * v + j:4 * v + j + 1] = jnp.sum(racc[j], axis=0, keepdims=True)
                if last:
                    rtx[it, 8 + 4 * v + j:8 + 4 * v + j + 1] = jnp.sum(tacc[j], axis=0, keepdims=True)
        if it == 0:
            for i in range(8):
                rtx[it, 8 + i:9 + i] = dsum[i]
        nrow = 8 if it == 1 else 16
        cps = [send(rtx.at[it, 0:nrow], rrx.at[it, j, 0:nrow], rs.at[it, j], rr.at[it, j], j, 0) for j in range(1, np_)]
        background(it, False)
        rtot = rtx[it, 0:nrow]
        for j, cp in zip(range(1, np_), cps):
            cp.wait_recv()
            rtot = rtot + rrx[it, j, 0:nrow]
        if it == 0:
            dfull = rtot[8:16]
        u_tile = 1.0 / (total_rows * rtot[0:8])
        if not last:
            for v in range(2):
                cols = []
                for ck in range(B // CH):
                    rows = pl.ds(ck * CH, CH)
                    part = None
                    for j in range(4):
                        m = A[v, rows, j * L:(j + 1) * L] * u_tile[4 * v + j:4 * v + j + 1]
                        part = m if part is None else part + m
                    cols.append(jnp.sum(part, axis=1, keepdims=True))
                finish_cols(v, cols)

    w = total_rows * u_tile
    logd = jnp.log(dfull)
    swapped = jnp.concatenate([logd[4:8], logd[0:4]], axis=0)
    terms = w * rtot[8:16] * LN2 - (w * rtot[0:8]) * swapped
    tot = jnp.sum(jnp.sum(terms, axis=1, keepdims=True), axis=0, keepdims=True)
    rowv[d, 0:8] = w
    rowv[d, 8:16] = 1.0 / dfull
    rowv[d, 16:24] = jnp.broadcast_to(tot, (8, L))
    ucps = [send(rowv.at[d], rowv.at[d], us.at[j], ur.at[j], 0, j) for j in range(1, nd)]
    background(ITERS, True)
    for cp in ucps + vcps:
        cp.wait_recv()
    for cp in pend:
        cp.wait_send()


def grads_kernel(np_, nd, zall, call, E, ET, rowv, vvec, vrep, q1, q2, loss, g1, g2, gp,
                 H, ucol, qbuf, sem):
    p = lax.axis_index('proto')
    d = lax.axis_index('data')
    total_rows = nd * B
    inv_scale = 1.0 / (2 * total_rows * TEMP_TAU)
    eye = eye_mask()
    lsum = rowv[0, 16:17, 0:1]
    for k in range(1, nd):
        lsum = lsum + rowv[k, 16:17, 0:1]
    loss[...] = lsum * (-1.0 / (2 * total_rows))

    for i in range(16):
        ucol[i // 4, (i % 4) * L:(i % 4 + 1) * L] = jnp.broadcast_to(
            row_to_col(eye, rowv[d, i:i + 1]) * inv_scale, (L, L))

    vt = vvec[p]
    out = []
    for h in range(2):
        for ck in range(B // CH):
            rows = pl.ds(ck * CH, CH)
            for j in range(2):
                lanes = slice(j * L, (j + 1) * L)
                for v in range(2):
                    e = E[v, 2 * p + h, rows, lanes]
                    vrow = vt[4 * v + 2 * h + j:4 * v + 2 * h + j + 1] * (1.0 / inv_scale)
                    qbuf[v, rows, h * HB + j * L:h * HB + (j + 1) * L] = (e * e) * vrow * ucol[v, rows]
    out = [pltpu.make_async_copy(qbuf.at[0], q1, sem.at[0]), pltpu.make_async_copy(qbuf.at[1], q2, sem.at[1])]
    for cp in out:
        cp.start()

    def form_rows(hb, slot):
        vq = vvec[hb // 2]
        par = lax.rem(hb, 2) == 0
        vl = [jnp.where(par, vq[4 * (i // 2) + i % 2:4 * (i // 2) + i % 2 + 1],
                        vq[4 * (i // 2) + 2 + i % 2:4 * (i // 2) + 3 + i % 2]) for i in range(4)]
        for ck in range(B // CH):
            rows = pl.ds(ck * CH, CH)
            for j in range(2):
                lanes = slice(j * L, (j + 1) * L)
                e1 = E[0, hb, rows, lanes]
                e2 = E[1, hb, rows, lanes]
                a1 = (e1 * e1) * vl[j] * ucol[0, rows]
                a2 = (e2 * e2) * vl[2 + j] * ucol[1, rows]
                H[slot, 0, rows, lanes] = (e1 * ucol[2, rows] - a2).astype(BF16)
                H[slot, 1, rows, lanes] = (e2 * ucol[3, rows] - a1).astype(BF16)

    g1[...] = jnp.zeros_like(g1)
    g2[...] = jnp.zeros_like(g2)
    gp[...] = jnp.zeros_like(gp)
    n_hb = 2 * np_
    form_rows(0, 0)

    def row_step(i, carry):
        for s in range(2):
            hb = 2 * i + s
            cb = call[hb]
            g1[...] += jnp.dot(H[s, 0], cb, preferred_element_type=F32)
            g2[...] += jnp.dot(H[s, 1], cb, preferred_element_type=F32)
            form_rows(lax.rem(hb + 1, n_hb), 1 - s)
        return carry

    lax.fori_loop(0, np_, row_step, 0)

    def form_cols(nb, slot):
        rv = rowv[nb // 2, 0:16] * inv_scale
        par = lax.rem(nb, 2) == 0
        rl = [jnp.where(par, rv[4 * (i // 2) + i % 2:4 * (i // 2) + i % 2 + 1],
                        rv[4 * (i // 2) + 2 + i % 2:4 * (i // 2) + 3 + i % 2]) for i in range(8)]
        for ck in range(B // CH):
            rows = pl.ds(ck * CH, CH)
            for j in range(2):
                lanes = slice(j * L, (j + 1) * L)
                e1 = ET[0, nb, rows, lanes]
                e2 = ET[1, nb, rows, lanes]
                a1 = (e1 * e1) * rl[j] * vrep[0, rows]
                a2 = (e2 * e2) * rl[2 + j] * vrep[1, rows]
                H[slot, 0, rows, lanes] = (e1 * rl[4 + j] - a2).astype(BF16)
                H[slot, 1, rows, lanes] = (e2 * rl[6 + j] - a1).astype(BF16)

    n_nb = 2 * nd
    form_cols(0, 0)

    def col_step(i, carry):
        for s in range(2):
            nb = 2 * i + s
            gp[...] += (jnp.dot(H[s, 0], zall[0, nb], preferred_element_type=F32)
                        + jnp.dot(H[s, 1], zall[1, nb], preferred_element_type=F32))
            form_cols(lax.rem(nb + 1, n_nb), 1 - s)
        return carry

    lax.fori_loop(0, nd, col_step, 0)
    for cp in out:
        cp.wait()


def solution(mesh):
    np_ = mesh.shape['proto']
    nd = mesh.shape['data']
    VM = pl.BlockSpec(memory_space=pltpu.VMEM)
    HBM = pl.BlockSpec(memory_space=pltpu.HBM)
    ANY = pl.BlockSpec(memory_space=pl.ANY)
    DMA = pltpu.SemaphoreType.DMA

    def local_step(emb_one, emb_two, protos):
        dim = protos.shape[1]
        mid = pl.pallas_call(
            functools.partial(sinkhorn_kernel, np_, nd),
            out_shape=(jax.ShapeDtypeStruct((2, 2 * nd, HB, dim), BF16),
                       jax.ShapeDtypeStruct((2 * np_, HB, dim), BF16),
                       jax.ShapeDtypeStruct((2, 2 * np_, B, HB), F32),
                       jax.ShapeDtypeStruct((2, 2 * nd, B, HB), F32),
                       jax.ShapeDtypeStruct((nd, 24, L), F32), jax.ShapeDtypeStruct((np_, 8, L), F32),
                       jax.ShapeDtypeStruct((2, B, L), F32)),
            in_specs=[HBM] * 3, out_specs=(VM,) * 7,
            scratch_shapes=[
                pltpu.VMEM((2, B, B), F32), pltpu.VMEM((2, B, B), F32),
                pltpu.VMEM((ITERS, 8, L), F32), pltpu.VMEM((ITERS, nd, 8, L), F32),
                pltpu.VMEM((ITERS, 16, L), F32), pltpu.VMEM((ITERS, np_, 16, L), F32),
                DMA((6,)), DMA((ITERS, nd)), DMA((ITERS, nd)), DMA((ITERS, np_)), DMA((ITERS, np_)),
                DMA((np_,)), DMA((np_,)), DMA((nd,)), DMA((nd,)),
                DMA((12,)), DMA((12,)), DMA((9,)), DMA((9,)), DMA((np_,)), DMA((np_,))],
            compiler_params=pltpu.CompilerParams(collective_id=0, has_side_effects=True, vmem_limit_bytes=12 << 20),
            name='sinkhorn',
        )(*[pltpu.with_memory_space_constraint(a, pltpu.HBM) for a in (emb_one, emb_two, protos)])
        q1, q2, loss, g1, g2, gp = pl.pallas_call(
            functools.partial(grads_kernel, np_, nd),
            out_shape=(jax.ShapeDtypeStruct((B, B), F32), jax.ShapeDtypeStruct((B, B), F32),
                       jax.ShapeDtypeStruct((1, 1), F32),
                       jax.ShapeDtypeStruct((B, dim), F32), jax.ShapeDtypeStruct((B, dim), F32),
                       jax.ShapeDtypeStruct((B, dim), F32)),
            in_specs=[VM] * 7, out_specs=(ANY, ANY, VM, VM, VM, VM),
            scratch_shapes=[pltpu.VMEM((2, 2, B, HB), BF16), pltpu.VMEM((4, B, L), F32),
                            pltpu.VMEM((2, B, B), F32), DMA((2,))],
            compiler_params=pltpu.CompilerParams(vmem_limit_bytes=12 << 20),
            name='grads',
        )(*mid)
        return q1, q2, loss.reshape(()), g1, g2, gp

    return jax.shard_map(
        local_step, mesh=mesh,
        in_specs=(P('data', None), P('data', None), P('proto', None)),
        out_specs=(P('data', 'proto'), P('data', 'proto'), P(), P('data', None), P('data', None), P('proto', None)),
        check_vma=False)
```

```python
import functools
import math

import jax
import jax.numpy as jnp
from jax import lax
from jax.experimental import pallas as pl
from jax.experimental.pallas import tpu as pltpu
from jax.sharding import PartitionSpec as P

TEMP_TAU = 0.1
ITERS = 3
F32, BF16 = jnp.float32, jnp.bfloat16
LOG2E_TAU = math.log2(math.e) / TEMP_TAU
LN2 = math.log(2.0)
B = 512
HB = 256
L = 128
CH = 64
EARLY = 4
RC = 16
NT = (((1,), (1,)), ((), ()))


def eye_mask():
    return lax.broadcasted_iota(jnp.int32, (L, L), 0) == lax.broadcasted_iota(jnp.int32, (L, L), 1)


def col_to_row(eye, col):
    return jnp.sum(jnp.where(eye, col, 0.0), axis=0, keepdims=True)


def row_to_col(eye, row):
    return jnp.sum(jnp.where(eye, row, 0.0), axis=1, keepdims=True)


def xor(a, k):
    out = a
    for bit in (1, 2, 4):
        if k & bit:
            out = out + bit - 2 * bit * lax.rem(out // bit, 2)
    return out


def xor2(a, b):
    out = 0
    for bit in (1, 2, 4):
        out = out + bit * lax.rem(lax.rem(a // bit, 2) + lax.rem(b // bit, 2), 2)
    return out


def form_rows(E, vvec, ucol, H, q):
    vq = vvec[q]
    for ck in range(B // RC):
        rows = pl.ds(ck * RC, RC)
        u1, u2 = ucol[0, rows], ucol[1, rows]
        for j in range(4):
            lanes = slice((j % 2) * L, (j % 2 + 1) * L)
            p1 = E[0, 2 * q + j // 2, rows, lanes]
            p2 = E[1, 2 * q + j // 2, rows, lanes]
            a1 = (p1 * p1) * u1 * vq[j:j + 1]
            a2 = (p2 * p2) * u2 * vq[4 + j:5 + j]
            H[0, rows, j * L:(j + 1) * L] = (p1 - a2).astype(BF16)
            H[1, rows, j * L:(j + 1) * L] = (p2 - a1).astype(BF16)


def dz_blocks(E, vvec, ucol, H, call, G, p, lo, hi, first):
    form_rows(E, vvec, ucol, H.at[0], xor2(p, lo))
    if first:
        G[...] = jnp.zeros_like(G)

    def two(i, carry):
        for s in range(2):
            j = lo + 2 * i + s
            q = xor2(p, j)
            for v in range(2):
                G[v] += times_block(H.at[s], v, call, q)
            form_rows(E, vvec, ucol, H.at[1 - s], xor2(p, lax.rem(j + 1, 8)))
        return carry

    lax.fori_loop(0, (hi - lo) // 2, two, 0)


def times_block(H, v, call, q):
    return jnp.dot(H[v], call[pl.ds(2 * q, 2)].reshape(B, -1), preferred_element_type=F32)


def sinkhorn_kernel(np_, nd, z1, z2, c, zall, call, E, ET, rowv, vvec, vrep, ucol, G,
                    T, A, H, dall, ctx, crx, rtx, rrx,
                    lsem, cs, cr, rs, rr, vs, vr, us, ur, zs, zr, gs, gr, ds_, dr_):
    p = lax.axis_index('proto')
    d = lax.axis_index('data')
    total_rows = nd * B
    total_protos = np_ * B
    inv_scale = 1.0 / (2 * total_rows * TEMP_TAU)
    half = lax.rem(d, 2)
    other = 1 - half

    loads = [pltpu.make_async_copy(z1.at[h * HB:(h + 1) * HB], zall.at[0, 2 * d + h], lsem.at[h]) for h in range(2)]
    loads += [pltpu.make_async_copy(z2.at[h * HB:(h + 1) * HB], zall.at[1, 2 * d + h], lsem.at[2 + h]) for h in range(2)]
    loads += [pltpu.make_async_copy(c.at[h * HB:(h + 1) * HB], call.at[2 * p + h], lsem.at[4 + h]) for h in range(2)]
    for cp in loads:
        cp.start()

    dp = [xor(d, j) for j in range(nd)]
    pp = [xor(p, j) for j in range(np_)]

    bar = pltpu.get_barrier_semaphore()
    for j in range(1, nd):
        pl.semaphore_signal(bar, inc=1, device_id={'proto': p, 'data': dp[j]})
    for j in range(1, np_):
        pl.semaphore_signal(bar, inc=1, device_id={'proto': pp[j], 'data': d})

    for cp in loads:
        cp.wait()

    pend = []

    def send(src, dst, ss, rs_, pj, dj):
        cp = pltpu.make_async_remote_copy(src, dst, ss, rs_, device_id={'proto': pp[pj], 'data': dp[dj]})
        cp.start()
        pend.append(cp)
        return cp

    def z_x(i):
        ref = zall.at[i // 2, 2 * d + i % 2]
        return send(ref, ref, zs.at[i], zr.at[i], 0, 2)

    def z_partner(slot, v, nb):
        ref = zall.at[v, nb]
        return send(ref, ref, zs.at[slot], zr.at[slot], 0, 1)

    def c_send(slot, q, pj):
        ref = call.at[2 * q + half]
        return send(ref, ref, gs.at[slot], gr.at[slot], pj, 0)

    def c_partner(j):
        ref = call.at[2 * pp[j] + half]
        return send(ref, ref, ds_.at[j], dr_.at[j], 0, 1)

    def own_images(v):
        return zall[v, pl.ds(2 * d, 2)].reshape(B, -1)

    def own_protos():
        return call[pl.ds(2 * p, 2)].reshape(B, -1)

    def scores_rows(hb):
        for v in range(2):
            s = lax.dot_general(own_images(v), call[hb], NT, preferred_element_type=F32)
            for j in range(2):
                lanes = slice(j * L, (j + 1) * L)
                E[v, hb, :, lanes] = jnp.exp2(s[:, lanes] * LOG2E_TAU) * ucol[2 + v]

    def scores_cols(nb):
        for v in range(2):
            s = lax.dot_general(own_protos(), zall[v, nb], NT, preferred_element_type=F32)
            for j in range(2):
                lanes = slice(j * L, (j + 1) * L)
                row = pl.ds(4 * v + 2 * lax.rem(nb, 2) + j, 1)
                ET[v, nb, :, lanes] = jnp.exp2(s[:, lanes] * LOG2E_TAU) * dall[nb // 2, row]

    eye = eye_mask()

    crow = [None] * 8
    dsum = [None] * 8
    for v in range(2):
        dacc = [None] * 4
        for h in range(2):
            part = None
            for h2 in range(2):
                s = lax.dot_general(call[2 * p + h], zall[v, 2 * d + h2], NT, preferred_element_type=F32)
                e = jnp.exp2(s * LOG2E_TAU)
                A[v, h * HB:(h + 1) * HB, h2 * HB:(h2 + 1) * HB] = e
                a = e * e
                for j in range(2):
                    lanes = slice(j * L, (j + 1) * L)
                    ds = jnp.sum(e[:, lanes].reshape(HB // 8, 8, L), axis=0)
                    k = 2 * h2 + j
                    dacc[k] = ds if dacc[k] is None else dacc[k] + ds
                    part = a[:, lanes] if part is None else part + a[:, lanes]
            col = jnp.sum(part, axis=1, keepdims=True)
            for i in range(2):
                crow[4 * v + 2 * h + i] = col_to_row(eye, col[i * L:(i + 1) * L])
        for j in range(4):
            dsum[4 * v + j] = jnp.sum(dacc[j], axis=0, keepdims=True)

    pl.semaphore_wait(bar, nd - 1 + np_ - 1)

    bulk = {}

    def background(it, along_data):
        if it == 0 and along_data:
            bulk['y0'] = c_send(0, p, 1)
            bulk['z2'] = c_send(1, p, 2)
            bulk['zx', 0] = z_x(0)
            for v in range(2):
                for h in range(2):
                    bulk['zp', v, h] = z_partner(4 + 2 * v + h, v, 2 * d + h)
            for v in range(2):
                for ck in range(B // CH):
                    rows = pl.ds(ck * CH, CH)
                    e = A[v, rows]
                    for h in range(2):
                        ET[v, 2 * d + h, rows] = e[:, h * HB:(h + 1) * HB]
                    A[v, rows] = e * e
            for v in range(2):
                T[v] = lax.dot_general(own_protos(), own_images(v), NT, preferred_element_type=F32) * LOG2E_TAU
        elif it == 0:
            bulk['z4'] = c_send(2, p, 4)
            bulk['zx', 1] = z_x(1)
            bulk['y0'].wait_recv()
            bulk['d1'] = c_partner(1)
            bulk['z2'].wait_recv()
            bulk['y2'] = c_send(4, pp[2], 1)
            bulk['d2'] = c_partner(2)
        elif it == 1 and along_data:
            bulk['zx', 2] = z_x(2)
            for i in range(8):
                ucol[2 + i // 4, (i % 4) * L:(i % 4 + 1) * L] = jnp.broadcast_to(
                    row_to_col(eye, dscale[i:i + 1]), (L, L))
            scores_rows(2 * p)
            scores_rows(2 * p + 1)
            scores_rows(2 * pp[1] + half)
        elif it == 1:
            bulk['z6'] = c_send(3, p, 6)
            bulk['zx', 3] = z_x(3)
            bulk['z4'].wait_recv()
            bulk['y4'] = c_send(5, pp[4], 1)
            bulk['d4'] = c_partner(4)
            bulk['y2'].wait_recv()
            bulk['d3'] = c_partner(3)
            scores_rows(2 * pp[2] + half)
            for j in (1, 2):
                bulk['d%d' % j].wait_recv()
                scores_rows(2 * pp[j] + other)
            for v in range(2):
                for h in range(2):
                    bulk['zp', v, h].wait_recv()
            scores_cols(2 * dp[1])
            scores_cols(2 * dp[1] + 1)
            scores_rows(2 * pp[4] + half)
            scores_rows(2 * pp[3] + half)
            for v in range(2):
                for h in range(2):
                    for j in range(2):
                        lanes = slice(j * L, (j + 1) * L)
                        k = 4 * v + 2 * h + j
                        ET[v, 2 * d + h, :, lanes] = ET[v, 2 * d + h, :, lanes] * dscale[k:k + 1]
        elif it == 2 and along_data:
            for j in (4, 3):
                bulk['d%d' % j].wait_recv()
                scores_rows(2 * pp[j] + other)
            for i in range(4):
                bulk['zx', i].wait_recv()
                bulk['zf', i] = z_partner(8 + i, i // 2, 2 * dp[2] + i % 2)
            scores_cols(2 * dp[2])
            scores_cols(2 * dp[2] + 1)
        elif it == 2:
            bulk['z6'].wait_recv()
            bulk['y6'] = c_send(6, pp[6], 1)
            bulk['d6'] = c_partner(6)
            bulk['y4'].wait_recv()
            bulk['d5'] = c_partner(5)
            for i in range(4):
                bulk['zf', i].wait_recv()
            scores_cols(2 * dp[3])
            scores_cols(2 * dp[3] + 1)
            for j in (6, 5):
                scores_rows(2 * pp[j] + half)
                bulk['d%d' % j].wait_recv()
                scores_rows(2 * pp[j] + other)
        else:
            for i in range(8):
                ucol[i // 4, (i % 4) * L:(i % 4 + 1) * L] = jnp.broadcast_to(
                    row_to_col(eye, useg[i:i + 1]), (L, L))
            for cp in vcps:
                cp.wait_recv()
            dz_blocks(E, vvec, ucol, H, call, G, p, 0, EARLY, True)
            bulk['y6'].wait_recv()
            bulk['d7'] = c_partner(7)
            scores_rows(2 * pp[7] + half)
            bulk['d7'].wait_recv()
            scores_rows(2 * pp[7] + other)

    for it in range(ITERS):
        last = it == ITERS - 1
        for i in range(8):
            ctx[it, i:i + 1] = crow[i]
        nc = 8
        if it == 1:
            nc = 16
            ctx[it, 8:16] = dscale
        cps = [send(ctx.at[it, 0:nc], crx.at[it, j, 0:nc], cs.at[it, j], cr.at[it, j], 0, j) for j in range(1, nd)]
        background(it, True)
        ctot = ctx[it, 0:8]
        for j, cp in zip(range(1, nd), cps):
            cp.wait_recv()
            ctot = ctot + crx[it, j, 0:8]
        if it == 1:
            dall[d] = dscale
            for j in range(1, nd):
                dall[dp[j]] = crx[it, j, 8:16]
        vt = 1.0 / (total_protos * ctot)
        if last:
            vvec[p] = vt
            vcps = [send(vvec.at[p], vvec.at[p], vs.at[j], vr.at[j], j, 0) for j in range(1, np_)]
        for v in range(2):
            for i in range(4):
                vrep[v, i * L:(i + 1) * L] = jnp.broadcast_to(row_to_col(eye, vt[4 * v + i:4 * v + i + 1]), (L, L))
        for v in range(2):
            racc = [jnp.zeros((8, L), F32) for _ in range(4)]
            tacc = [jnp.zeros((8, L), F32) for _ in range(4)]
            for ck in range(B // CH):
                rows = pl.ds(ck * CH, CH)
                wv = vrep[v, rows]
                for j in range(4):
                    lanes = slice(j * L, (j + 1) * L)
                    m = A[v, rows, lanes] * wv
                    racc[j] = racc[j] + jnp.sum(m.reshape(CH // 8, 8, L), axis=0)
                    if last:
                        mt = m * T[1 - v, rows, lanes]
                        tacc[j] = tacc[j] + jnp.sum(mt.reshape(CH // 8, 8, L), axis=0)
            for j in range(4):
                rtx[it, 4 * v + j:4 * v + j + 1] = jnp.sum(racc[j], axis=0, keepdims=True)
                if last:
                    rtx[it, 8 + 4 * v + j:8 + 4 * v + j + 1] = jnp.sum(tacc[j], axis=0, keepdims=True)
        if it == 0:
            for i in range(8):
                rtx[it, 8 + i:9 + i] = dsum[i]
        nrow = 8 if it == 1 else 16
        cps = [send(rtx.at[it, 0:nrow], rrx.at[it, j, 0:nrow], rs.at[it, j], rr.at[it, j], j, 0) for j in range(1, np_)]
        background(it, False)
        rtot = rtx[it, 0:nrow]
        for j, cp in zip(range(1, np_), cps):
            cp.wait_recv()
            rtot = rtot + rrx[it, j, 0:nrow]
        if it == 0:
            dfull = rtot[8:16]
            dscale = inv_scale / dfull
        u_tile = 1.0 / (total_rows * rtot[0:8])
        if not last:
            for v in range(2):
                cols = []
                for ck in range(B // CH):
                    rows = pl.ds(ck * CH, CH)
                    part = None
                    for j in range(4):
                        m = A[v, rows, j * L:(j + 1) * L] * u_tile[4 * v + j:4 * v + j + 1]
                        part = m if part is None else part + m
                    cols.append(jnp.sum(part, axis=1, keepdims=True))
                per = L // CH
                for i in range(4):
                    crow[4 * v + i] = col_to_row(eye, jnp.concatenate(cols[per * i:per * (i + 1)], axis=0))

    w = total_rows * u_tile
    logd = jnp.log(dfull)
    swapped = jnp.concatenate([logd[4:8], logd[0:4]], axis=0)
    terms = w * rtot[8:16] * LN2 - (w * rtot[0:8]) * swapped
    tot = jnp.sum(jnp.sum(terms, axis=1, keepdims=True), axis=0, keepdims=True)
    useg = w * inv_scale / (dscale * dscale)
    rowv[d, 0:8] = useg
    rowv[d, 8:16] = jnp.broadcast_to(tot, (8, L))
    ucps = [send(rowv.at[d], rowv.at[d], us.at[j], ur.at[j], 0, j) for j in range(1, nd)]
    background(ITERS, True)
    for cp in ucps:
        cp.wait_recv()
    for cp in pend:
        cp.wait_send()


def grads_kernel(np_, nd, zall, call, E, ET, rowv, vvec, vrep, ucol, G, q1, q2, loss, g1, g2, gp,
                 H, qbuf, gbuf, gsum, sem):
    p = lax.axis_index('proto')
    d = lax.axis_index('data')
    total_rows = nd * B
    scale = 2 * total_rows * TEMP_TAU
    inv_scale = 1.0 / scale
    lsum = rowv[0, 8:9, 0:1]
    for k in range(1, nd):
        lsum = lsum + rowv[k, 8:9, 0:1]
    loss[...] = lsum * (-1.0 / (2 * total_rows))

    vt = vvec[p] * scale

    def codes(ck, carry):
        rows = pl.ds(pl.multiple_of(ck * CH, CH), CH)
        for v in range(2):
            uv = ucol[v, rows]
            for j in range(4):
                e = E[v, 2 * p + j // 2, rows, (j % 2) * L:(j % 2 + 1) * L]
                qbuf[v, rows, j * L:(j + 1) * L] = (e * e) * uv * vt[4 * v + j:4 * v + j + 1]
        return carry

    lax.fori_loop(0, B // CH, codes, 0)
    out = [pltpu.make_async_copy(qbuf.at[0], q1, sem.at[0]), pltpu.make_async_copy(qbuf.at[1], q2, sem.at[1])]
    for cp in out:
        cp.start()

    gbuf[0:2] = G[...]
    dz_blocks(E, vvec, ucol, H, call, gbuf, p, EARLY, np_, False)
    gout = [pltpu.make_async_copy(gbuf.at[0], g1, sem.at[2]), pltpu.make_async_copy(gbuf.at[1], g2, sem.at[3])]
    for cp in gout:
        cp.start()

    def form_cols(Hs, k):
        rv = rowv[k, 0:8]
        for ck in range(B // RC):
            rows = pl.ds(ck * RC, RC)
            v1, v2 = vrep[0, rows], vrep[1, rows]
            for j in range(4):
                lanes = slice((j % 2) * L, (j % 2 + 1) * L)
                p1 = ET[0, 2 * k + j // 2, rows, lanes]
                p2 = ET[1, 2 * k + j // 2, rows, lanes]
                a1 = (p1 * p1) * rv[j:j + 1] * v1
                a2 = (p2 * p2) * rv[4 + j:5 + j] * v2
                Hs[0, rows, j * L:(j + 1) * L] = (p1 - a2).astype(BF16)
                Hs[1, rows, j * L:(j + 1) * L] = (p2 - a1).astype(BF16)

    form_cols(H.at[0], 0)
    gsum[...] = jnp.zeros_like(gsum)

    def two(i, carry):
        for s in range(2):
            k = 2 * i + s
            t = [jnp.dot(H[s, v], zall[v, pl.ds(2 * k, 2)].reshape(B, -1), preferred_element_type=F32) for v in range(2)]
            gsum[...] += t[0] + t[1]
            form_cols(H.at[1 - s], lax.rem(k + 1, nd))
        return carry

    lax.fori_loop(0, nd // 2, two, 0)
    gout.append(pltpu.make_async_copy(gsum, gp, sem.at[4]))
    gout[-1].start()
    for cp in out + gout:
        cp.wait()


def solution(mesh):
    np_ = mesh.shape['proto']
    nd = mesh.shape['data']
    VM = pl.BlockSpec(memory_space=pltpu.VMEM)
    HBM = pl.BlockSpec(memory_space=pltpu.HBM)
    ANY = pl.BlockSpec(memory_space=pl.ANY)
    DMA = pltpu.SemaphoreType.DMA

    def local_step(emb_one, emb_two, protos):
        dim = protos.shape[1]
        sds = jax.ShapeDtypeStruct
        mid = pl.pallas_call(
            functools.partial(sinkhorn_kernel, np_, nd),
            out_shape=(sds((2, 2 * nd, HB, dim), BF16), sds((2 * np_, HB, dim), BF16),
                       sds((2, 2 * np_, B, HB), F32), sds((2, 2 * nd, B, HB), F32),
                       sds((nd, 16, L), F32), sds((np_, 8, L), F32),
                       sds((2, B, L), F32), sds((4, B, L), F32), sds((2, B, dim), F32)),
            in_specs=[HBM] * 3, out_specs=(VM,) * 9,
            scratch_shapes=[
                pltpu.VMEM((2, B, B), F32), pltpu.VMEM((2, B, B), F32), pltpu.VMEM((2, 2, B, B), BF16),
                pltpu.VMEM((nd, 8, L), F32),
                pltpu.VMEM((ITERS, 16, L), F32), pltpu.VMEM((ITERS, nd, 16, L), F32),
                pltpu.VMEM((ITERS, 16, L), F32), pltpu.VMEM((ITERS, np_, 16, L), F32),
                DMA((6,)), DMA((ITERS, nd)), DMA((ITERS, nd)), DMA((ITERS, np_)), DMA((ITERS, np_)),
                DMA((np_,)), DMA((np_,)), DMA((nd,)), DMA((nd,)),
                DMA((12,)), DMA((12,)), DMA((7,)), DMA((7,)), DMA((np_,)), DMA((np_,))],
            compiler_params=pltpu.CompilerParams(collective_id=0, has_side_effects=True, vmem_limit_bytes=10 << 20),
            name='sinkhorn',
        )(*[pltpu.with_memory_space_constraint(a, pltpu.HBM) for a in (emb_one, emb_two, protos)])
        q1, q2, loss, g1, g2, gp = pl.pallas_call(
            functools.partial(grads_kernel, np_, nd),
            out_shape=(sds((B, B), F32), sds((B, B), F32), sds((1, 1), F32),
                       sds((B, dim), F32), sds((B, dim), F32), sds((B, dim), F32)),
            in_specs=[VM] * 9, out_specs=(ANY, ANY, VM, ANY, ANY, ANY),
            scratch_shapes=[pltpu.VMEM((2, 2, B, B), BF16), pltpu.VMEM((2, B, B), F32),
                            pltpu.VMEM((2, B, dim), F32), pltpu.VMEM((B, dim), F32), DMA((5,))],
            compiler_params=pltpu.CompilerParams(vmem_limit_bytes=17 << 20),
            name='grads',
        )(*mid)
        return q1, q2, loss.reshape(()), g1, g2, gp

    return jax.shard_map(
        local_step, mesh=mesh,
        in_specs=(P('data', None), P('data', None), P('proto', None)),
        out_specs=(P('data', 'proto'), P('data', 'proto'), P(), P('data', None), P('data', None), P('proto', None)),
        check_vma=False)
```

```python
import functools
import math

import jax
import jax.numpy as jnp
from jax import lax
from jax.experimental import pallas as pl
from jax.experimental.pallas import tpu as pltpu
from jax.sharding import PartitionSpec as P

TEMP_TAU = 0.1
ITERS = 3
F32, BF16 = jnp.float32, jnp.bfloat16
LOG2E_TAU = math.log2(math.e) / TEMP_TAU
LN2 = math.log(2.0)
B = 512
HB = 256
L = 128
CH = 64
EARLY = 4
RC = 16
NT = (((1,), (1,)), ((), ()))


def eye_mask():
    return lax.broadcasted_iota(jnp.int32, (L, L), 0) == lax.broadcasted_iota(jnp.int32, (L, L), 1)


def col_to_row(eye, col):
    return jnp.sum(jnp.where(eye, col, 0.0), axis=0, keepdims=True)


def row_to_col(eye, row):
    return jnp.sum(jnp.where(eye, row, 0.0), axis=1, keepdims=True)


def xor(a, k):
    out = a
    for bit in (1, 2, 4):
        if k & bit:
            out = out + bit - 2 * bit * lax.rem(out // bit, 2)
    return out


def xor2(a, b):
    out = 0
    for bit in (1, 2, 4):
        out = out + bit * lax.rem(lax.rem(a // bit, 2) + lax.rem(b // bit, 2), 2)
    return out


def form_rows(E, vvec, ucol, H, q):
    vq = vvec[q]
    for ck in range(B // RC):
        rows = pl.ds(ck * RC, RC)
        u1, u2 = ucol[0, rows], ucol[1, rows]
        for j in range(4):
            lanes = slice((j % 2) * L, (j % 2 + 1) * L)
            p1 = E[0, 2 * q + j // 2, rows, lanes]
            p2 = E[1, 2 * q + j // 2, rows, lanes]
            a1 = (p1 * p1) * u1 * vq[j:j + 1]
            a2 = (p2 * p2) * u2 * vq[4 + j:5 + j]
            H[0, j, rows] = (p1 - a2).astype(BF16)
            H[1, j, rows] = (p2 - a1).astype(BF16)


def dz_blocks(E, vvec, ucol, H, call, G, p, lo, hi, first):
    form_rows(E, vvec, ucol, H.at[0], xor2(p, lo))
    if first:
        G[...] = jnp.zeros_like(G)

    def two(i, carry):
        for s in range(2):
            j = lo + 2 * i + s
            q = xor2(p, j)
            for v in range(2):
                G[v] += times_block(H.at[s], v, call, q)
            form_rows(E, vvec, ucol, H.at[1 - s], xor2(p, lax.rem(j + 1, 8)))
        return carry

    lax.fori_loop(0, (hi - lo) // 2, two, 0)


def slabs(H, v):
    return jnp.concatenate([H[v, j] for j in range(4)], axis=1)


def times_block(H, v, call, q):
    return jnp.dot(slabs(H, v), call[pl.ds(2 * q, 2)].reshape(B, -1), preferred_element_type=F32)


def sinkhorn_kernel(np_, nd, z1, z2, c, zall, call, E, ET, rowv, vvec, vrep, ucol, G,
                    T, A, H, dall, ctx, crx, rtx, rrx,
                    lsem, cs, cr, rs, rr, vs, vr, us, ur, zs, zr, gs, gr, ds_, dr_):
    p = lax.axis_index('proto')
    d = lax.axis_index('data')
    total_rows = nd * B
    total_protos = np_ * B
    inv_scale = 1.0 / (2 * total_rows * TEMP_TAU)
    half = lax.rem(d, 2)
    other = 1 - half

    loads = [pltpu.make_async_copy(z1.at[h * HB:(h + 1) * HB], zall.at[0, 2 * d + h], lsem.at[h]) for h in range(2)]
    loads += [pltpu.make_async_copy(z2.at[h * HB:(h + 1) * HB], zall.at[1, 2 * d + h], lsem.at[2 + h]) for h in range(2)]
    loads += [pltpu.make_async_copy(c.at[h * HB:(h + 1) * HB], call.at[2 * p + h], lsem.at[4 + h]) for h in range(2)]
    for cp in loads:
        cp.start()

    dp = [xor(d, j) for j in range(nd)]
    pp = [xor(p, j) for j in range(np_)]

    bar = pltpu.get_barrier_semaphore()
    for j in range(1, nd):
        pl.semaphore_signal(bar, inc=1, device_id={'proto': p, 'data': dp[j]})
    for j in range(1, np_):
        pl.semaphore_signal(bar, inc=1, device_id={'proto': pp[j], 'data': d})

    for cp in loads:
        cp.wait()

    pend = []

    def send(src, dst, ss, rs_, pj, dj):
        cp = pltpu.make_async_remote_copy(src, dst, ss, rs_, device_id={'proto': pp[pj], 'data': dp[dj]})
        cp.start()
        pend.append(cp)
        return cp

    def z_x(i):
        ref = zall.at[i // 2, 2 * d + i % 2]
        return send(ref, ref, zs.at[i], zr.at[i], 0, 2)

    def z_partner(slot, v, nb):
        ref = zall.at[v, nb]
        return send(ref, ref, zs.at[slot], zr.at[slot], 0, 1)

    def c_send(slot, q, pj, part=None):
        ref = call.at[2 * q + half]
        if part is not None:
            ref = ref.at[part * L:(part + 1) * L]
        return send(ref, ref, gs.at[slot], gr.at[slot], pj, 0)

    def c_partner(j):
        ref = call.at[2 * pp[j] + half]
        return send(ref, ref, ds_.at[j], dr_.at[j], 0, 1)

    def own_images(v):
        return zall[v, pl.ds(2 * d, 2)].reshape(B, -1)

    def own_protos():
        return call[pl.ds(2 * p, 2)].reshape(B, -1)

    def scores_rows(hb):
        for v in range(2):
            s = lax.dot_general(own_images(v), call[hb], NT, preferred_element_type=F32)
            for j in range(2):
                lanes = slice(j * L, (j + 1) * L)
                E[v, hb, :, lanes] = jnp.exp2(s[:, lanes] * LOG2E_TAU) * ucol[2 + v]

    def scores_cols(nb):
        for v in range(2):
            s = lax.dot_general(own_protos(), zall[v, nb], NT, preferred_element_type=F32)
            for j in range(2):
                lanes = slice(j * L, (j + 1) * L)
                row = pl.ds(4 * v + 2 * lax.rem(nb, 2) + j, 1)
                ET[v, nb, :, lanes] = jnp.exp2(s[:, lanes] * LOG2E_TAU) * dall[nb // 2, row]

    eye = eye_mask()

    crow = [None] * 8
    dsum = [None] * 8
    for v in range(2):
        dacc = [None] * 4
        for h in range(2):
            part = None
            for h2 in range(2):
                s = lax.dot_general(call[2 * p + h], zall[v, 2 * d + h2], NT, preferred_element_type=F32)
                e = jnp.exp2(s * LOG2E_TAU)
                A[v, h * HB:(h + 1) * HB, h2 * HB:(h2 + 1) * HB] = e
                a = e * e
                for j in range(2):
                    lanes = slice(j * L, (j + 1) * L)
                    ds = jnp.sum(e[:, lanes].reshape(HB // 8, 8, L), axis=0)
                    k = 2 * h2 + j
                    dacc[k] = ds if dacc[k] is None else dacc[k] + ds
                    part = a[:, lanes] if part is None else part + a[:, lanes]
            col = jnp.sum(part, axis=1, keepdims=True)
            for i in range(2):
                crow[4 * v + 2 * h + i] = col_to_row(eye, col[i * L:(i + 1) * L])
        for j in range(4):
            dsum[4 * v + j] = jnp.sum(dacc[j], axis=0, keepdims=True)

    pl.semaphore_wait(bar, nd - 1 + np_ - 1)

    bulk = {}

    def background(it, along_data):
        if it == 0 and along_data:
            bulk['y0'] = c_send(0, p, 1)
            bulk['z4', 0] = c_send(2, p, 4, 0)
            bulk['z2'] = c_send(1, p, 2)
            bulk['zx', 0] = z_x(0)
            for v in range(2):
                for h in range(2):
                    bulk['zp', v, h] = z_partner(4 + 2 * v + h, v, 2 * d + h)
            for v in range(2):
                for ck in range(B // CH):
                    rows = pl.ds(ck * CH, CH)
                    e = A[v, rows]
                    for h in range(2):
                        ET[v, 2 * d + h, rows] = e[:, h * HB:(h + 1) * HB]
                    A[v, rows] = e * e
            for v in range(2):
                T[v] = lax.dot_general(own_protos(), own_images(v), NT, preferred_element_type=F32) * LOG2E_TAU
        elif it == 0:
            bulk['zx', 1] = z_x(1)
            bulk['y0'].wait_recv()
            bulk['d1'] = c_partner(1)
            bulk['z2'].wait_recv()
            bulk['y2'] = c_send(4, pp[2], 1)
            bulk['d2'] = c_partner(2)
        elif it == 1 and along_data:
            bulk['z4', 1] = c_send(3, p, 4, 1)
            bulk['z6', 0] = c_send(7, p, 6, 0)
            bulk['zx', 2] = z_x(2)
            for i in range(8):
                ucol[2 + i // 4, (i % 4) * L:(i % 4 + 1) * L] = jnp.broadcast_to(
                    row_to_col(eye, dscale[i:i + 1]), (L, L))
            scores_rows(2 * p)
            scores_rows(2 * p + 1)
            scores_rows(2 * pp[1] + half)
        elif it == 1:
            bulk['zx', 3] = z_x(3)
            bulk['z4', 0].wait_recv()
            bulk['z4', 1].wait_recv()
            bulk['y4'] = c_send(5, pp[4], 1)
            bulk['d4'] = c_partner(4)
            bulk['y2'].wait_recv()
            bulk['d3'] = c_partner(3)
            scores_rows(2 * pp[2] + half)
            for j in (1, 2):
                bulk['d%d' % j].wait_recv()
                scores_rows(2 * pp[j] + other)
            for v in range(2):
                for h in range(2):
                    bulk['zp', v, h].wait_recv()
            scores_cols(2 * dp[1])
            scores_cols(2 * dp[1] + 1)
            scores_rows(2 * pp[4] + half)
            scores_rows(2 * pp[3] + half)
            bulk['z6', 0].wait_recv()
            bulk['y6', 0] = c_send(6, pp[6], 1, 0)
            for v in range(2):
                for h in range(2):
                    for j in range(2):
                        lanes = slice(j * L, (j + 1) * L)
                        k = 4 * v + 2 * h + j
                        ET[v, 2 * d + h, :, lanes] = ET[v, 2 * d + h, :, lanes] * dscale[k:k + 1]
        elif it == 2 and along_data:
            bulk['z6', 1] = c_send(8, p, 6, 1)
            for j in (4, 3):
                bulk['d%d' % j].wait_recv()
                scores_rows(2 * pp[j] + other)
            for i in range(4):
                bulk['zx', i].wait_recv()
                bulk['zf', i] = z_partner(8 + i, i // 2, 2 * dp[2] + i % 2)
            scores_cols(2 * dp[2])
            scores_cols(2 * dp[2] + 1)
        elif it == 2:
            bulk['z6', 1].wait_recv()
            bulk['y6', 1] = c_send(9, pp[6], 1, 1)
            bulk['d6'] = c_partner(6)
            bulk['y4'].wait_recv()
            bulk['d5'] = c_partner(5)
            for i in range(4):
                bulk['zf', i].wait_recv()
            scores_cols(2 * dp[3])
            scores_cols(2 * dp[3] + 1)
            for j in (6, 5):
                scores_rows(2 * pp[j] + half)
                bulk['d%d' % j].wait_recv()
                scores_rows(2 * pp[j] + other)
        else:
            for i in range(8):
                ucol[i // 4, (i % 4) * L:(i % 4 + 1) * L] = jnp.broadcast_to(
                    row_to_col(eye, useg[i:i + 1]), (L, L))
            for cp in vcps:
                cp.wait_recv()
            dz_blocks(E, vvec, ucol, H, call, G, p, 0, EARLY, True)
            bulk['y6', 0].wait_recv()
            bulk['y6', 1].wait_recv()
            bulk['d7'] = c_partner(7)
            scores_rows(2 * pp[7] + half)
            bulk['d7'].wait_recv()
            scores_rows(2 * pp[7] + other)

    for it in range(ITERS):
        last = it == ITERS - 1
        for i in range(8):
            ctx[it, i:i + 1] = crow[i]
        nc = 8
        if it == 1:
            nc = 16
            ctx[it, 8:16] = dscale
        cps = [send(ctx.at[it, 0:nc], crx.at[it, j, 0:nc], cs.at[it, j], cr.at[it, j], 0, j) for j in range(1, nd)]
        background(it, True)
        ctot = ctx[it, 0:8]
        for j, cp in zip(range(1, nd), cps):
            cp.wait_recv()
            ctot = ctot + crx[it, j, 0:8]
        if it == 1:
            dall[d] = dscale
            for j in range(1, nd):
                dall[dp[j]] = crx[it, j, 8:16]
        vt = 1.0 / (total_protos * ctot)
        if last:
            vvec[p] = vt
            vcps = [send(vvec.at[p], vvec.at[p], vs.at[j], vr.at[j], j, 0) for j in range(1, np_)]
        for v in range(2):
            for i in range(4):
                vrep[v, i * L:(i + 1) * L] = jnp.broadcast_to(row_to_col(eye, vt[4 * v + i:4 * v + i + 1]), (L, L))
        for v in range(2):
            racc = [jnp.zeros((8, L), F32) for _ in range(4)]
            tacc = [jnp.zeros((8, L), F32) for _ in range(4)]
            for ck in range(B // CH):
                rows = pl.ds(ck * CH, CH)
                wv = vrep[v, rows]
                for j in range(4):
                    lanes = slice(j * L, (j + 1) * L)
                    m = A[v, rows, lanes] * wv
                    racc[j] = racc[j] + jnp.sum(m.reshape(CH // 8, 8, L), axis=0)
                    if last:
                        mt = m * T[1 - v, rows, lanes]
                        tacc[j] = tacc[j] + jnp.sum(mt.reshape(CH // 8, 8, L), axis=0)
            for j in range(4):
                rtx[it, 4 * v + j:4 * v + j + 1] = jnp.sum(racc[j], axis=0, keepdims=True)
                if last:
                    rtx[it, 8 + 4 * v + j:8 + 4 * v + j + 1] = jnp.sum(tacc[j], axis=0, keepdims=True)
        if it == 0:
            for i in range(8):
                rtx[it, 8 + i:9 + i] = dsum[i]
        nrow = 8 if it == 1 else 16
        cps = [send(rtx.at[it, 0:nrow], rrx.at[it, j, 0:nrow], rs.at[it, j], rr.at[it, j], j, 0) for j in range(1, np_)]
        background(it, False)
        rtot = rtx[it, 0:nrow]
        for j, cp in zip(range(1, np_), cps):
            cp.wait_recv()
            rtot = rtot + rrx[it, j, 0:nrow]
        if it == 0:
            dfull = rtot[8:16]
            dscale = inv_scale / dfull
        u_tile = 1.0 / (total_rows * rtot[0:8])
        if not last:
            for v in range(2):
                cols = []
                for ck in range(B // CH):
                    rows = pl.ds(ck * CH, CH)
                    part = None
                    for j in range(4):
                        m = A[v, rows, j * L:(j + 1) * L] * u_tile[4 * v + j:4 * v + j + 1]
                        part = m if part is None else part + m
                    cols.append(jnp.sum(part, axis=1, keepdims=True))
                per = L // CH
                for i in range(4):
                    crow[4 * v + i] = col_to_row(eye, jnp.concatenate(cols[per * i:per * (i + 1)], axis=0))

    w = total_rows * u_tile
    logd = jnp.log(dfull)
    swapped = jnp.concatenate([logd[4:8], logd[0:4]], axis=0)
    terms = w * rtot[8:16] * LN2 - (w * rtot[0:8]) * swapped
    tot = jnp.sum(jnp.sum(terms, axis=1, keepdims=True), axis=0, keepdims=True)
    useg = w * inv_scale / (dscale * dscale)
    rowv[d, 0:8] = useg
    rowv[d, 8:16] = jnp.broadcast_to(tot, (8, L))
    ucps = [send(rowv.at[d], rowv.at[d], us.at[j], ur.at[j], 0, j) for j in range(1, nd)]
    background(ITERS, True)
    for cp in ucps:
        cp.wait_recv()
    for cp in pend:
        cp.wait_send()


def grads_kernel(np_, nd, zall, call, E, ET, rowv, vvec, vrep, ucol, G, q1, q2, loss, g1, g2, gp,
                 H, qbuf, gbuf, gsum, sem):
    p = lax.axis_index('proto')
    d = lax.axis_index('data')
    total_rows = nd * B
    scale = 2 * total_rows * TEMP_TAU
    inv_scale = 1.0 / scale
    lsum = rowv[0, 8:9, 0:1]
    for k in range(1, nd):
        lsum = lsum + rowv[k, 8:9, 0:1]
    loss[...] = lsum * (-1.0 / (2 * total_rows))

    vt = vvec[p] * scale

    def codes(ck, carry):
        rows = pl.ds(pl.multiple_of(ck * CH, CH), CH)
        for v in range(2):
            uv = ucol[v, rows]
            for j in range(4):
                e = E[v, 2 * p + j // 2, rows, (j % 2) * L:(j % 2 + 1) * L]
                qbuf[v, rows, j * L:(j + 1) * L] = (e * e) * uv * vt[4 * v + j:4 * v + j + 1]
        return carry

    lax.fori_loop(0, B // CH, codes, 0)
    out = [pltpu.make_async_copy(qbuf.at[0], q1, sem.at[0]), pltpu.make_async_copy(qbuf.at[1], q2, sem.at[1])]
    for cp in out:
        cp.start()

    gbuf[0:2] = G[...]
    dz_blocks(E, vvec, ucol, H, call, gbuf, p, EARLY, np_, False)
    gout = [pltpu.make_async_copy(gbuf.at[0], g1, sem.at[2]), pltpu.make_async_copy(gbuf.at[1], g2, sem.at[3])]
    for cp in gout:
        cp.start()

    def form_cols(Hs, k):
        rv = rowv[k, 0:8]
        for ck in range(B // RC):
            rows = pl.ds(ck * RC, RC)
            v1, v2 = vrep[0, rows], vrep[1, rows]
            for j in range(4):
                lanes = slice((j % 2) * L, (j % 2 + 1) * L)
                p1 = ET[0, 2 * k + j // 2, rows, lanes]
                p2 = ET[1, 2 * k + j // 2, rows, lanes]
                a1 = (p1 * p1) * rv[j:j + 1] * v1
                a2 = (p2 * p2) * rv[4 + j:5 + j] * v2
                Hs[0, j, rows] = (p1 - a2).astype(BF16)
                Hs[1, j, rows] = (p2 - a1).astype(BF16)

    form_cols(H.at[0], 0)
    gsum[...] = jnp.zeros_like(gsum)

    def two(i, carry):
        for s in range(2):
            k = 2 * i + s
            t = [jnp.dot(slabs(H.at[s], v), zall[v, pl.ds(2 * k, 2)].reshape(B, -1), preferred_element_type=F32) for v in range(2)]
            gsum[...] += t[0] + t[1]
            form_cols(H.at[1 - s], lax.rem(k + 1, nd))
        return carry

    lax.fori_loop(0, nd // 2, two, 0)
    gout.append(pltpu.make_async_copy(gsum, gp, sem.at[4]))
    gout[-1].start()
    for cp in out + gout:
        cp.wait()


def solution(mesh):
    np_ = mesh.shape['proto']
    nd = mesh.shape['data']
    VM = pl.BlockSpec(memory_space=pltpu.VMEM)
    HBM = pl.BlockSpec(memory_space=pltpu.HBM)
    ANY = pl.BlockSpec(memory_space=pl.ANY)
    DMA = pltpu.SemaphoreType.DMA

    def local_step(emb_one, emb_two, protos):
        dim = protos.shape[1]
        sds = jax.ShapeDtypeStruct
        mid = pl.pallas_call(
            functools.partial(sinkhorn_kernel, np_, nd),
            out_shape=(sds((2, 2 * nd, HB, dim), BF16), sds((2 * np_, HB, dim), BF16),
                       sds((2, 2 * np_, B, HB), F32), sds((2, 2 * nd, B, HB), F32),
                       sds((nd, 16, L), F32), sds((np_, 8, L), F32),
                       sds((2, B, L), F32), sds((4, B, L), F32), sds((2, B, dim), F32)),
            in_specs=[HBM] * 3, out_specs=(VM,) * 9,
            scratch_shapes=[
                pltpu.VMEM((2, B, B), F32), pltpu.VMEM((2, B, B), F32), pltpu.VMEM((2, 2, 4, B, L), BF16),
                pltpu.VMEM((nd, 8, L), F32),
                pltpu.VMEM((ITERS, 16, L), F32), pltpu.VMEM((ITERS, nd, 16, L), F32),
                pltpu.VMEM((ITERS, 16, L), F32), pltpu.VMEM((ITERS, np_, 16, L), F32),
                DMA((6,)), DMA((ITERS, nd)), DMA((ITERS, nd)), DMA((ITERS, np_)), DMA((ITERS, np_)),
                DMA((np_,)), DMA((np_,)), DMA((nd,)), DMA((nd,)),
                DMA((12,)), DMA((12,)), DMA((10,)), DMA((10,)), DMA((np_,)), DMA((np_,))],
            compiler_params=pltpu.CompilerParams(collective_id=0, has_side_effects=True, vmem_limit_bytes=10 << 20),
            name='sinkhorn',
        )(*[pltpu.with_memory_space_constraint(a, pltpu.HBM) for a in (emb_one, emb_two, protos)])
        q1, q2, loss, g1, g2, gp = pl.pallas_call(
            functools.partial(grads_kernel, np_, nd),
            out_shape=(sds((B, B), F32), sds((B, B), F32), sds((1, 1), F32),
                       sds((B, dim), F32), sds((B, dim), F32), sds((B, dim), F32)),
            in_specs=[VM] * 9, out_specs=(ANY, ANY, VM, ANY, ANY, ANY),
            scratch_shapes=[pltpu.VMEM((2, 2, 4, B, L), BF16), pltpu.VMEM((2, B, B), F32),
                            pltpu.VMEM((2, B, dim), F32), pltpu.VMEM((B, dim), F32), DMA((5,))],
            compiler_params=pltpu.CompilerParams(vmem_limit_bytes=17 << 20),
            name='grads',
        )(*mid)
        return q1, q2, loss.reshape(()), g1, g2, gp

    return jax.shard_map(
        local_step, mesh=mesh,
        in_specs=(P('data', None), P('data', None), P('proto', None)),
        out_specs=(P('data', 'proto'), P('data', 'proto'), P(), P('data', None), P('data', None), P('proto', None)),
        check_vma=False)
```

```python
import functools
import math

import jax
import jax.numpy as jnp
from jax import lax
from jax.experimental import pallas as pl
from jax.experimental.pallas import tpu as pltpu
from jax.sharding import PartitionSpec as P

TEMP_TAU = 0.1
ITERS = 3
F32, BF16 = jnp.float32, jnp.bfloat16
LOG2E_TAU = math.log2(math.e) / TEMP_TAU
LN2 = math.log(2.0)
B = 512
HB = 256
L = 128
CH = 64
EARLY = 6
RC = 16
NT = (((1,), (1,)), ((), ()))


def eye_mask():
    return lax.broadcasted_iota(jnp.int32, (L, L), 0) == lax.broadcasted_iota(jnp.int32, (L, L), 1)


def col_to_row(eye, col):
    return jnp.sum(jnp.where(eye, col, 0.0), axis=0, keepdims=True)


def row_to_col(eye, row):
    return jnp.sum(jnp.where(eye, row, 0.0), axis=1, keepdims=True)


def xor(a, k):
    out = a
    for bit in (1, 2, 4):
        if k & bit:
            out = out + bit - 2 * bit * lax.rem(out // bit, 2)
    return out


def xor2(a, b):
    out = 0
    for bit in (1, 2, 4):
        out = out + bit * lax.rem(lax.rem(a // bit, 2) + lax.rem(b // bit, 2), 2)
    return out


def form_rows(E, vvec, ucol, H, q):
    vq = vvec[q]
    for ck in range(B // RC):
        rows = pl.ds(ck * RC, RC)
        u1, u2 = ucol[0, rows], ucol[1, rows]
        for j in range(4):
            lanes = slice((j % 2) * L, (j % 2 + 1) * L)
            p1 = E[0, 2 * q + j // 2, rows, lanes]
            p2 = E[1, 2 * q + j // 2, rows, lanes]
            a1 = (p1 * p1) * u1 * vq[j:j + 1]
            a2 = (p2 * p2) * u2 * vq[4 + j:5 + j]
            H[0, j, rows] = (p1 - a2).astype(BF16)
            H[1, j, rows] = (p2 - a1).astype(BF16)


def dz_blocks(E, vvec, ucol, H, call, G, p, lo, hi, first):
    form_rows(E, vvec, ucol, H.at[0], xor2(p, lo))
    if first:
        G[...] = jnp.zeros_like(G)

    def two(i, carry):
        for s in range(2):
            j = lo + 2 * i + s
            q = xor2(p, j)
            for v in range(2):
                G[v] += times_block(H.at[s], v, call, q)
            form_rows(E, vvec, ucol, H.at[1 - s], xor2(p, lax.rem(j + 1, 8)))
        return carry

    lax.fori_loop(0, (hi - lo) // 2, two, 0)


def slabs(H, v):
    return jnp.concatenate([H[v, j] for j in range(4)], axis=1)


def times_block(H, v, call, q):
    return jnp.dot(slabs(H, v), call[pl.ds(2 * q, 2)].reshape(B, -1), preferred_element_type=F32)


def sinkhorn_kernel(np_, nd, z1, z2, c, zall, call, E, ET, rowv, vvec, vrep, ucol, G,
                    T, A, H, dall, ctx, crx, rtx, rrx, dtx, drx, ttx, trx,
                    lsem, cs, cr, rs, rr, vs, vr, us, ur, ts, tr, zs, zr, gs, gr, ds_, dr_):
    p = lax.axis_index('proto')
    d = lax.axis_index('data')
    total_rows = nd * B
    total_protos = np_ * B
    inv_scale = 1.0 / (2 * total_rows * TEMP_TAU)
    half = lax.rem(d, 2)
    other = 1 - half

    loads = [pltpu.make_async_copy(z1.at[h * HB:(h + 1) * HB], zall.at[0, 2 * d + h], lsem.at[h]) for h in range(2)]
    loads += [pltpu.make_async_copy(z2.at[h * HB:(h + 1) * HB], zall.at[1, 2 * d + h], lsem.at[2 + h]) for h in range(2)]
    loads += [pltpu.make_async_copy(c.at[h * HB:(h + 1) * HB], call.at[2 * p + h], lsem.at[4 + h]) for h in range(2)]
    for cp in loads:
        cp.start()

    dp = [xor(d, j) for j in range(nd)]
    pp = [xor(p, j) for j in range(np_)]

    bar = pltpu.get_barrier_semaphore()
    for j in range(1, nd):
        pl.semaphore_signal(bar, inc=1, device_id={'proto': p, 'data': dp[j]})
    for j in range(1, np_):
        pl.semaphore_signal(bar, inc=1, device_id={'proto': pp[j], 'data': d})

    for cp in loads:
        cp.wait()

    pend = []

    def send(src, dst, ss, rs_, pj, dj):
        cp = pltpu.make_async_remote_copy(src, dst, ss, rs_, device_id={'proto': pp[pj], 'data': dp[dj]})
        cp.start()
        pend.append(cp)
        return cp

    def z_x(i):
        ref = zall.at[i // 2, 2 * d + i % 2]
        return send(ref, ref, zs.at[i], zr.at[i], 0, 2)

    def z_partner(slot, v, nb):
        ref = zall.at[v, nb]
        return send(ref, ref, zs.at[slot], zr.at[slot], 0, 1)

    quarter = pl.ds(pl.multiple_of(d // 2 * L, L), L)

    def c_send(slot, q, pj, dj=0, whole=False):
        ref = call.at[2 * q + half] if whole else call.at[2 * q + half, quarter]
        return send(ref, ref, gs.at[slot], gr.at[slot], pj, dj)

    def c_partner(j):
        ref = call.at[2 * pp[j] + half]
        return send(ref, ref, ds_.at[j], dr_.at[j], 0, 1)

    def own_images(v):
        return zall[v, pl.ds(2 * d, 2)].reshape(B, -1)

    def own_protos():
        return call[pl.ds(2 * p, 2)].reshape(B, -1)

    def scores_rows(hb):
        for v in range(2):
            s = lax.dot_general(own_images(v), call[hb], NT, preferred_element_type=F32)
            for j in range(2):
                lanes = slice(j * L, (j + 1) * L)
                E[v, hb, :, lanes] = jnp.exp2(s[:, lanes] * LOG2E_TAU) * ucol[2 + v]

    def scores_cols(nb):
        for v in range(2):
            s = lax.dot_general(own_protos(), zall[v, nb], NT, preferred_element_type=F32)
            for j in range(2):
                lanes = slice(j * L, (j + 1) * L)
                row = pl.ds(4 * v + 2 * lax.rem(nb, 2) + j, 1)
                ET[v, nb, :, lanes] = jnp.exp2(s[:, lanes] * LOG2E_TAU) * dall[nb // 2, row]

    eye = eye_mask()

    crow = [None] * 8
    dsum = [None] * 8
    for v in range(2):
        dacc = [None] * 4
        for h in range(2):
            part = None
            for h2 in range(2):
                s = lax.dot_general(call[2 * p + h], zall[v, 2 * d + h2], NT, preferred_element_type=F32)
                e = jnp.exp2(s * LOG2E_TAU)
                A[v, h * HB:(h + 1) * HB, h2 * HB:(h2 + 1) * HB] = e
                a = e * e
                for j in range(2):
                    lanes = slice(j * L, (j + 1) * L)
                    ds = jnp.sum(e[:, lanes].reshape(HB // 8, 8, L), axis=0)
                    k = 2 * h2 + j
                    dacc[k] = ds if dacc[k] is None else dacc[k] + ds
                    part = a[:, lanes] if part is None else part + a[:, lanes]
            col = jnp.sum(part, axis=1, keepdims=True)
            for i in range(2):
                crow[4 * v + 2 * h + i] = col_to_row(eye, col[i * L:(i + 1) * L])
        for j in range(4):
            dsum[4 * v + j] = jnp.sum(dacc[j], axis=0, keepdims=True)

    pl.semaphore_wait(bar, nd - 1 + np_ - 1)

    bulk = {}

    def c_x(j):
        bulk['x', j] = c_send(7 + j, pp[j], 0, 2)

    def have(*keys):
        for key in keys:
            bulk[key].wait_recv()

    def hand_on(j):
        bulk['d', j] = c_partner(j)

    def background(it, along_data):
        if it == 0 and along_data:
            bulk['y', 0] = c_send(0, p, 1, whole=True)
            bulk['z', 2] = c_send(1, p, 2)
            bulk['z', 4] = c_send(2, p, 4)
            bulk['zx', 0] = z_x(0)
            for i in range(4):
                bulk['zp', i] = z_partner(4 + i, i // 2, 2 * d + i % 2)
            for v in range(2):
                for ck in range(B // CH):
                    rows = pl.ds(ck * CH, CH)
                    e = A[v, rows]
                    for h in range(2):
                        ET[v, 2 * d + h, rows] = e[:, h * HB:(h + 1) * HB]
                    A[v, rows] = e * e
            for v in range(2):
                T[v] = lax.dot_general(own_protos(), own_images(v), NT, preferred_element_type=F32) * LOG2E_TAU
        elif it == 0:
            bulk['zx', 1] = z_x(1)
            have(('z', 2))
            c_x(2)
            bulk['y', 2] = c_send(4, pp[2], 1)
            have(('y', 0))
            hand_on(1)
            have(('z', 4))
            bulk['y', 4] = c_send(5, pp[4], 1)
        elif it == 1 and along_data:
            bulk['z', 6] = c_send(3, p, 6)
            c_x(4)
            have(('y', 2))
            c_x(3)
            bulk['zx', 2] = z_x(2)
            have(('y', 4))
            c_x(5)
            for i in range(8):
                ucol[2 + i // 4, (i % 4) * L:(i % 4 + 1) * L] = jnp.broadcast_to(
                    row_to_col(eye, dscale[i:i + 1]), (L, L))
            scores_rows(2 * p)
            scores_rows(2 * p + 1)
            have(('x', 2))
            hand_on(2)
            scores_rows(2 * pp[1] + half)
        elif it == 1:
            have(('x', 4))
            hand_on(4)
            have(('d', 1))
            scores_rows(2 * pp[1] + other)
            scores_rows(2 * pp[2] + half)
            have(('d', 2))
            scores_rows(2 * pp[2] + other)
            have(('z', 6))
            c_x(6)
            bulk['y', 6] = c_send(6, pp[6], 1)
            have(('zp', 0), ('zp', 1), ('zp', 2), ('zp', 3))
            scores_cols(2 * dp[1])
            scores_cols(2 * dp[1] + 1)
            for v in range(2):
                for h in range(2):
                    for j in range(2):
                        lanes = slice(j * L, (j + 1) * L)
                        k = 4 * v + 2 * h + j
                        ET[v, 2 * d + h, :, lanes] = ET[v, 2 * d + h, :, lanes] * dscale[k:k + 1]
            scores_rows(2 * pp[4] + half)
        elif it == 2 and along_data:
            bulk['zx', 3] = z_x(3)
            have(('x', 3))
            hand_on(3)
            have(('x', 5))
            hand_on(5)
            have(('d', 4))
            scores_rows(2 * pp[4] + other)
            for i in range(3):
                have(('zx', i))
                bulk['zf', i] = z_partner(8 + i, i // 2, 2 * dp[2] + i % 2)
            scores_rows(2 * pp[3] + half)
            scores_rows(2 * pp[5] + half)
        elif it == 2:
            have(('y', 6))
            c_x(7)
            have(('x', 6))
            hand_on(6)
            have(('zx', 3))
            bulk['zf', 3] = z_partner(11, 1, 2 * dp[2] + 1)
            for j in (3, 5):
                have(('d', j))
                scores_rows(2 * pp[j] + other)
            scores_cols(2 * dp[2])
            scores_cols(2 * dp[2] + 1)
            have(('zf', 0), ('zf', 1), ('zf', 2), ('zf', 3))
            scores_cols(2 * dp[3])
            scores_cols(2 * dp[3] + 1)
            have(('x', 7))
            hand_on(7)
            scores_rows(2 * pp[6] + half)
            have(('d', 6))
            scores_rows(2 * pp[6] + other)
            scores_rows(2 * pp[7] + half)
            have(('d', 7))
            scores_rows(2 * pp[7] + other)

    def sum_tiles(own, parts, cps):
        tot = own[...]
        for j, cp in zip(range(1, np_), cps):
            cp.wait_recv()
            tot = tot + parts[j]
        return tot

    def row_tile(own, parts, ss, rs_):
        return [send(own, parts.at[j], ss.at[j], rs_.at[j], j, 0) for j in range(1, np_)]

    for it in range(ITERS):
        last = it == ITERS - 1
        for i in range(8):
            ctx[it, i:i + 1] = crow[i]
        nc = 8
        if it == 1:
            nc = 16
            dfull = sum_tiles(dtx, drx, dcps)
            dscale = inv_scale / dfull
            ctx[it, 8:16] = dscale
        cps = [send(ctx.at[it, 0:nc], crx.at[it, j, 0:nc], cs.at[it, j], cr.at[it, j], 0, j) for j in range(1, nd)]
        background(it, True)
        ctot = ctx[it, 0:8]
        for j, cp in zip(range(1, nd), cps):
            cp.wait_recv()
            ctot = ctot + crx[it, j, 0:8]
        if it == 1:
            dall[d] = dscale
            for j in range(1, nd):
                dall[dp[j]] = crx[it, j, 8:16]
        vt = 1.0 / (total_protos * ctot)
        for v in range(2):
            for i in range(4):
                vrep[v, i * L:(i + 1) * L] = jnp.broadcast_to(row_to_col(eye, vt[4 * v + i:4 * v + i + 1]), (L, L))
        for v in range(2):
            racc = [jnp.zeros((8, L), F32) for _ in range(4)]
            for ck in range(B // CH):
                rows = pl.ds(ck * CH, CH)
                wv = vrep[v, rows]
                for j in range(4):
                    m = A[v, rows, j * L:(j + 1) * L] * wv
                    racc[j] = racc[j] + jnp.sum(m.reshape(CH // 8, 8, L), axis=0)
            for j in range(4):
                rtx[it, 4 * v + j:4 * v + j + 1] = jnp.sum(racc[j], axis=0, keepdims=True)
        cps = row_tile(rtx.at[it], rrx.at[it], rs.at[it], rr.at[it])
        if it == 0:
            for i in range(8):
                dtx[i:i + 1] = dsum[i]
            dcps = row_tile(dtx, drx, ts.at[0], tr.at[0])
        if last:
            vvec[p] = vt
            vcps = [send(vvec.at[p], vvec.at[p], vs.at[j], vr.at[j], j, 0) for j in range(1, np_)]
            for v in range(2):
                tacc = [jnp.zeros((8, L), F32) for _ in range(4)]
                for ck in range(B // CH):
                    rows = pl.ds(ck * CH, CH)
                    wv = vrep[v, rows]
                    for j in range(4):
                        lanes = slice(j * L, (j + 1) * L)
                        mt = A[v, rows, lanes] * wv * T[1 - v, rows, lanes]
                        tacc[j] = tacc[j] + jnp.sum(mt.reshape(CH // 8, 8, L), axis=0)
                for j in range(4):
                    ttx[4 * v + j:4 * v + j + 1] = jnp.sum(tacc[j], axis=0, keepdims=True)
            tcps = row_tile(ttx, trx, ts.at[1], tr.at[1])
        background(it, False)
        rtot = sum_tiles(rtx.at[it], rrx.at[it], cps)
        u_tile = 1.0 / (total_rows * rtot)
        if not last:
            for v in range(2):
                cols = []
                for ck in range(B // CH):
                    rows = pl.ds(ck * CH, CH)
                    part = None
                    for j in range(4):
                        m = A[v, rows, j * L:(j + 1) * L] * u_tile[4 * v + j:4 * v + j + 1]
                        part = m if part is None else part + m
                    cols.append(jnp.sum(part, axis=1, keepdims=True))
                per = L // CH
                for i in range(4):
                    crow[4 * v + i] = col_to_row(eye, jnp.concatenate(cols[per * i:per * (i + 1)], axis=0))

    w = total_rows * u_tile
    useg = w * inv_scale / (dscale * dscale)
    rowv[d, 0:8] = useg
    ucps = [send(rowv.at[d, 0:8], rowv.at[d, 0:8], us.at[0, j], ur.at[0, j], 0, j) for j in range(1, nd)]
    for i in range(8):
        ucol[i // 4, (i % 4) * L:(i % 4 + 1) * L] = jnp.broadcast_to(row_to_col(eye, useg[i:i + 1]), (L, L))
    ttot = sum_tiles(ttx, trx, tcps)
    logd = jnp.log(dfull)
    swapped = jnp.concatenate([logd[4:8], logd[0:4]], axis=0)
    terms = w * ttot * LN2 - (w * rtot) * swapped
    tot = jnp.sum(jnp.sum(terms, axis=1, keepdims=True), axis=0, keepdims=True)
    rowv[d, 8:16] = jnp.broadcast_to(tot, (8, L))
    ucps += [send(rowv.at[d, 8:16], rowv.at[d, 8:16], us.at[1, j], ur.at[1, j], 0, j) for j in range(1, nd)]
    for cp in vcps:
        cp.wait_recv()
    dz_blocks(E, vvec, ucol, H, call, G, p, 0, EARLY, True)
    for cp in ucps:
        cp.wait_recv()
    for cp in pend:
        cp.wait_send()


def grads_kernel(np_, nd, zall, call, E, ET, rowv, vvec, vrep, ucol, G, q1, q2, loss, g1, g2, gp,
                 H, qbuf, gbuf, gsum, sem):
    p = lax.axis_index('proto')
    d = lax.axis_index('data')
    total_rows = nd * B
    scale = 2 * total_rows * TEMP_TAU
    inv_scale = 1.0 / scale
    lsum = rowv[0, 8:9, 0:1]
    for k in range(1, nd):
        lsum = lsum + rowv[k, 8:9, 0:1]
    loss[...] = lsum * (-1.0 / (2 * total_rows))

    vt = vvec[p] * scale

    def codes(ck, carry):
        rows = pl.ds(pl.multiple_of(ck * CH, CH), CH)
        for v in range(2):
            uv = ucol[v, rows]
            for j in range(4):
                e = E[v, 2 * p + j // 2, rows, (j % 2) * L:(j % 2 + 1) * L]
                qbuf[v, rows, j * L:(j + 1) * L] = (e * e) * uv * vt[4 * v + j:4 * v + j + 1]
        return carry

    lax.fori_loop(0, B // CH, codes, 0)
    out = [pltpu.make_async_copy(qbuf.at[0], q1, sem.at[0]), pltpu.make_async_copy(qbuf.at[1], q2, sem.at[1])]
    for cp in out:
        cp.start()

    gbuf[0:2] = G[...]
    dz_blocks(E, vvec, ucol, H, call, gbuf, p, EARLY, np_, False)
    gout = [pltpu.make_async_copy(gbuf.at[0], g1, sem.at[2]), pltpu.make_async_copy(gbuf.at[1], g2, sem.at[3])]
    for cp in gout:
        cp.start()

    def form_cols(Hs, k):
        rv = rowv[k, 0:8]
        for ck in range(B // RC):
            rows = pl.ds(ck * RC, RC)
            v1, v2 = vrep[0, rows], vrep[1, rows]
            for j in range(4):
                lanes = slice((j % 2) * L, (j % 2 + 1) * L)
                p1 = ET[0, 2 * k + j // 2, rows, lanes]
                p2 = ET[1, 2 * k + j // 2, rows, lanes]
                a1 = (p1 * p1) * rv[j:j + 1] * v1
                a2 = (p2 * p2) * rv[4 + j:5 + j] * v2
                Hs[0, j, rows] = (p1 - a2).astype(BF16)
                Hs[1, j, rows] = (p2 - a1).astype(BF16)

    form_cols(H.at[0], 0)
    gsum[...] = jnp.zeros_like(gsum)

    def two(i, carry):
        for s in range(2):
            k = 2 * i + s
            t = [jnp.dot(slabs(H.at[s], v), zall[v, pl.ds(2 * k, 2)].reshape(B, -1), preferred_element_type=F32) for v in range(2)]
            gsum[...] += t[0] + t[1]
            form_cols(H.at[1 - s], lax.rem(k + 1, nd))
        return carry

    lax.fori_loop(0, nd // 2, two, 0)
    gout.append(pltpu.make_async_copy(gsum, gp, sem.at[4]))
    gout[-1].start()
    for cp in out + gout:
        cp.wait()


def solution(mesh):
    np_ = mesh.shape['proto']
    nd = mesh.shape['data']
    VM = pl.BlockSpec(memory_space=pltpu.VMEM)
    HBM = pl.BlockSpec(memory_space=pltpu.HBM)
    ANY = pl.BlockSpec(memory_space=pl.ANY)
    DMA = pltpu.SemaphoreType.DMA

    def local_step(emb_one, emb_two, protos):
        dim = protos.shape[1]
        sds = jax.ShapeDtypeStruct
        mid = pl.pallas_call(
            functools.partial(sinkhorn_kernel, np_, nd),
            out_shape=(sds((2, 2 * nd, HB, dim), BF16), sds((2 * np_, HB, dim), BF16),
                       sds((2, 2 * np_, B, HB), F32), sds((2, 2 * nd, B, HB), F32),
                       sds((nd, 16, L), F32), sds((np_, 8, L), F32),
                       sds((2, B, L), F32), sds((4, B, L), F32), sds((2, B, dim), F32)),
            in_specs=[HBM] * 3, out_specs=(VM,) * 9,
            scratch_shapes=[
                pltpu.VMEM((2, B, B), F32), pltpu.VMEM((2, B, B), F32), pltpu.VMEM((2, 2, 4, B, L), BF16),
                pltpu.VMEM((nd, 8, L), F32),
                pltpu.VMEM((ITERS, 16, L), F32), pltpu.VMEM((ITERS, nd, 16, L), F32),
                pltpu.VMEM((ITERS, 8, L), F32), pltpu.VMEM((ITERS, np_, 8, L), F32),
                pltpu.VMEM((8, L), F32), pltpu.VMEM((np_, 8, L), F32), pltpu.VMEM((8, L), F32), pltpu.VMEM((np_, 8, L), F32),
                DMA((6,)), DMA((ITERS, nd)), DMA((ITERS, nd)), DMA((ITERS, np_)), DMA((ITERS, np_)),
                DMA((np_,)), DMA((np_,)), DMA((2, nd)), DMA((2, nd)), DMA((2, np_)), DMA((2, np_)),
                DMA((12,)), DMA((12,)), DMA((15,)), DMA((15,)), DMA((np_,)), DMA((np_,))],
            compiler_params=pltpu.CompilerParams(collective_id=0, has_side_effects=True, vmem_limit_bytes=10 << 20),
            name='sinkhorn',
        )(*[pltpu.with_memory_space_constraint(a, pltpu.HBM) for a in (emb_one, emb_two, protos)])
        q1, q2, loss, g1, g2, gp = pl.pallas_call(
            functools.partial(grads_kernel, np_, nd),
            out_shape=(sds((B, B), F32), sds((B, B), F32), sds((1, 1), F32),
                       sds((B, dim), F32), sds((B, dim), F32), sds((B, dim), F32)),
            in_specs=[VM] * 9, out_specs=(ANY, ANY, VM, ANY, ANY, ANY),
            scratch_shapes=[pltpu.VMEM((2, 2, 4, B, L), BF16), pltpu.VMEM((2, B, B), F32),
                            pltpu.VMEM((2, B, dim), F32), pltpu.VMEM((B, dim), F32), DMA((5,))],
            compiler_params=pltpu.CompilerParams(vmem_limit_bytes=17 << 20),
            name='grads',
        )(*mid)
        return q1, q2, loss.reshape(()), g1, g2, gp

    return jax.shard_map(
        local_step, mesh=mesh,
        in_specs=(P('data', None), P('data', None), P('proto', None)),
        out_specs=(P('data', 'proto'), P('data', 'proto'), P(), P('data', None), P('data', None), P('proto', None)),
        check_vma=False)
```

```python
import functools
import math

import jax
import jax.numpy as jnp
from jax import lax
from jax.experimental import pallas as pl
from jax.experimental.pallas import tpu as pltpu
from jax.sharding import PartitionSpec as P

TEMP_TAU = 0.1
ITERS = 3
F32, BF16 = jnp.float32, jnp.bfloat16
LOG2E_TAU = math.log2(math.e) / TEMP_TAU
LN2 = math.log(2.0)
B = 512
HB = 256
L = 128
CH = 64
RC = 16
NT = (((1,), (1,)), ((), ()))


def eye_mask():
    return lax.broadcasted_iota(jnp.int32, (L, L), 0) == lax.broadcasted_iota(jnp.int32, (L, L), 1)


def col_to_row(eye, col):
    return jnp.sum(jnp.where(eye, col, 0.0), axis=0, keepdims=True)


def row_to_col(eye, row):
    return jnp.sum(jnp.where(eye, row, 0.0), axis=1, keepdims=True)


def xor(a, k):
    out = a
    for bit in (1, 2, 4):
        if k & bit:
            out = out + bit - 2 * bit * lax.rem(out // bit, 2)
    return out


def xor2(a, b):
    out = 0
    for bit in (1, 2, 4):
        out = out + bit * lax.rem(lax.rem(a // bit, 2) + lax.rem(b // bit, 2), 2)
    return out


def form_rows(E, vvec, ucol, H, q):
    vq = vvec[q]
    for ck in range(B // RC):
        rows = pl.ds(ck * RC, RC)
        u1, u2 = ucol[0, rows], ucol[1, rows]
        for j in range(4):
            lanes = slice((j % 2) * L, (j % 2 + 1) * L)
            p1 = E[0, 2 * q + j // 2, rows, lanes]
            p2 = E[1, 2 * q + j // 2, rows, lanes]
            a1 = (p1 * p1) * u1 * vq[j:j + 1]
            a2 = (p2 * p2) * u2 * vq[4 + j:5 + j]
            H[0, j, rows] = (p1 - a2).astype(BF16)
            H[1, j, rows] = (p2 - a1).astype(BF16)


def dz_blocks(E, vvec, ucol, H, call, G, p, n):
    form_rows(E, vvec, ucol, H.at[0], p)
    G[...] = jnp.zeros_like(G)

    def two(i, carry):
        for s in range(2):
            j = 2 * i + s
            q = xor2(p, j)
            for v in range(2):
                G[v] += times_block(H.at[s], v, call, q)
            form_rows(E, vvec, ucol, H.at[1 - s], xor2(p, lax.rem(j + 1, 8)))
        return carry

    lax.fori_loop(0, n // 2, two, 0)


def slabs(H, v):
    return jnp.concatenate([H[v, j] for j in range(4)], axis=1)


def times_block(H, v, call, q):
    return jnp.dot(slabs(H, v), call[pl.ds(2 * q, 2)].reshape(B, -1), preferred_element_type=F32)


def sinkhorn_kernel(np_, nd, z1, z2, c, zall, call, E, ET, rowv, vvec, vrep, ucol, G,
                    T, A, H, dall, ctx, crx, rtx, rrx, dtx, drx, ttx, trx,
                    lsem, cs, cr, rs, rr, vs, vr, us, ur, ts, tr, zs, zr, gs, gr, ds_, dr_):
    p = lax.axis_index('proto')
    d = lax.axis_index('data')
    total_rows = nd * B
    total_protos = np_ * B
    inv_scale = 1.0 / (2 * total_rows * TEMP_TAU)
    half = lax.rem(d, 2)
    other = 1 - half

    loads = [pltpu.make_async_copy(z1.at[h * HB:(h + 1) * HB], zall.at[0, 2 * d + h], lsem.at[h]) for h in range(2)]
    loads += [pltpu.make_async_copy(z2.at[h * HB:(h + 1) * HB], zall.at[1, 2 * d + h], lsem.at[2 + h]) for h in range(2)]
    loads += [pltpu.make_async_copy(c.at[h * HB:(h + 1) * HB], call.at[2 * p + h], lsem.at[4 + h]) for h in range(2)]
    for cp in loads:
        cp.start()

    dp = [xor(d, j) for j in range(nd)]
    pp = [xor(p, j) for j in range(np_)]

    bar = pltpu.get_barrier_semaphore()
    for j in range(1, nd):
        pl.semaphore_signal(bar, inc=1, device_id={'proto': p, 'data': dp[j]})
    for j in range(1, np_):
        pl.semaphore_signal(bar, inc=1, device_id={'proto': pp[j], 'data': d})

    for cp in loads:
        cp.wait()

    pend = []

    def send(src, dst, ss, rs_, pj, dj):
        cp = pltpu.make_async_remote_copy(src, dst, ss, rs_, device_id={'proto': pp[pj], 'data': dp[dj]})
        cp.start()
        pend.append(cp)
        return cp

    def z_x(i):
        ref = zall.at[i // 2, 2 * d + i % 2]
        return send(ref, ref, zs.at[i], zr.at[i], 0, 2)

    def z_partner(slot, v, nb):
        ref = zall.at[v, nb]
        return send(ref, ref, zs.at[slot], zr.at[slot], 0, 1)

    quarter = pl.ds(pl.multiple_of(d // 2 * L, L), L)

    def c_send(slot, q, pj, dj=0, whole=False):
        ref = call.at[2 * q + half] if whole else call.at[2 * q + half, quarter]
        return send(ref, ref, gs.at[slot], gr.at[slot], pj, dj)

    def c_partner(j):
        ref = call.at[2 * pp[j] + half]
        return send(ref, ref, ds_.at[j], dr_.at[j], 0, 1)

    def own_images(v):
        return zall[v, pl.ds(2 * d, 2)].reshape(B, -1)

    def own_protos():
        return call[pl.ds(2 * p, 2)].reshape(B, -1)

    def scores_rows(hb):
        for v in range(2):
            s = lax.dot_general(own_images(v), call[hb], NT, preferred_element_type=F32)
            for j in range(2):
                lanes = slice(j * L, (j + 1) * L)
                E[v, hb, :, lanes] = jnp.exp2(s[:, lanes] * LOG2E_TAU) * ucol[2 + v]

    def scores_cols(nb):
        for v in range(2):
            s = lax.dot_general(own_protos(), zall[v, nb], NT, preferred_element_type=F32)
            for j in range(2):
                lanes = slice(j * L, (j + 1) * L)
                row = pl.ds(4 * v + 2 * lax.rem(nb, 2) + j, 1)
                ET[v, nb, :, lanes] = jnp.exp2(s[:, lanes] * LOG2E_TAU) * dall[nb // 2, row]

    eye = eye_mask()

    crow = [None] * 8
    dsum = [None] * 8
    for v in range(2):
        dacc = [None] * 4
        for h in range(2):
            part = None
            for h2 in range(2):
                s = lax.dot_general(call[2 * p + h], zall[v, 2 * d + h2], NT, preferred_element_type=F32)
                e = jnp.exp2(s * LOG2E_TAU)
                A[v, h * HB:(h + 1) * HB, h2 * HB:(h2 + 1) * HB] = e
                a = e * e
                for j in range(2):
                    lanes = slice(j * L, (j + 1) * L)
                    ds = jnp.sum(e[:, lanes].reshape(HB // 8, 8, L), axis=0)
                    k = 2 * h2 + j
                    dacc[k] = ds if dacc[k] is None else dacc[k] + ds
                    part = a[:, lanes] if part is None else part + a[:, lanes]
            col = jnp.sum(part, axis=1, keepdims=True)
            for i in range(2):
                crow[4 * v + 2 * h + i] = col_to_row(eye, col[i * L:(i + 1) * L])
        for j in range(4):
            dsum[4 * v + j] = jnp.sum(dacc[j], axis=0, keepdims=True)

    pl.semaphore_wait(bar, nd - 1 + np_ - 1)

    bulk = {}

    def c_x(j):
        bulk['x', j] = c_send(7 + j, pp[j], 0, 2)

    def have(*keys):
        for key in keys:
            bulk[key].wait_recv()

    def hand_on(j):
        bulk['d', j] = c_partner(j)

    def background(it, along_data):
        if it == 0 and along_data:
            bulk['y', 0] = c_send(0, p, 1, whole=True)
            bulk['z', 2] = c_send(1, p, 2)
            bulk['z', 4] = c_send(2, p, 4)
            bulk['zx', 0] = z_x(0)
            for i in range(4):
                bulk['zp', i] = z_partner(4 + i, i // 2, 2 * d + i % 2)
            for v in range(2):
                for ck in range(B // CH):
                    rows = pl.ds(ck * CH, CH)
                    e = A[v, rows]
                    for h in range(2):
                        ET[v, 2 * d + h, rows] = e[:, h * HB:(h + 1) * HB]
                    A[v, rows] = e * e
            for v in range(2):
                T[v] = lax.dot_general(own_protos(), own_images(v), NT, preferred_element_type=F32) * LOG2E_TAU
        elif it == 0:
            bulk['zx', 1] = z_x(1)
            have(('z', 2))
            c_x(2)
            bulk['y', 2] = c_send(4, pp[2], 1)
            have(('y', 0))
            hand_on(1)
            have(('z', 4))
            bulk['y', 4] = c_send(5, pp[4], 1)
        elif it == 1 and along_data:
            bulk['z', 6] = c_send(3, p, 6)
            c_x(4)
            have(('y', 2))
            c_x(3)
            bulk['zx', 2] = z_x(2)
            have(('y', 4))
            c_x(5)
            for i in range(8):
                ucol[2 + i // 4, (i % 4) * L:(i % 4 + 1) * L] = jnp.broadcast_to(
                    row_to_col(eye, dscale[i:i + 1]), (L, L))
            scores_rows(2 * p)
            scores_rows(2 * p + 1)
            have(('x', 2))
            hand_on(2)
            scores_rows(2 * pp[1] + half)
        elif it == 1:
            have(('x', 4))
            hand_on(4)
            have(('d', 1))
            scores_rows(2 * pp[1] + other)
            scores_rows(2 * pp[2] + half)
            have(('d', 2))
            scores_rows(2 * pp[2] + other)
            have(('z', 6))
            c_x(6)
            bulk['y', 6] = c_send(6, pp[6], 1)
            have(('zp', 0), ('zp', 1), ('zp', 2), ('zp', 3))
            scores_cols(2 * dp[1])
            scores_cols(2 * dp[1] + 1)
            for v in range(2):
                for h in range(2):
                    for j in range(2):
                        lanes = slice(j * L, (j + 1) * L)
                        k = 4 * v + 2 * h + j
                        ET[v, 2 * d + h, :, lanes] = ET[v, 2 * d + h, :, lanes] * dscale[k:k + 1]
            scores_rows(2 * pp[4] + half)
        elif it == 2 and along_data:
            bulk['zx', 3] = z_x(3)
            have(('x', 3))
            hand_on(3)
            have(('x', 5))
            hand_on(5)
            have(('d', 4))
            scores_rows(2 * pp[4] + other)
            for i in range(3):
                have(('zx', i))
                bulk['zf', i] = z_partner(8 + i, i // 2, 2 * dp[2] + i % 2)
            scores_rows(2 * pp[3] + half)
            scores_rows(2 * pp[5] + half)
        elif it == 2:
            have(('y', 6))
            c_x(7)
            have(('x', 6))
            hand_on(6)
            have(('zx', 3))
            bulk['zf', 3] = z_partner(11, 1, 2 * dp[2] + 1)
            for j in (3, 5):
                have(('d', j))
                scores_rows(2 * pp[j] + other)
            scores_cols(2 * dp[2])
            scores_cols(2 * dp[2] + 1)
            have(('zf', 0), ('zf', 1), ('zf', 2), ('zf', 3))
            scores_cols(2 * dp[3])
            scores_cols(2 * dp[3] + 1)
            have(('x', 7))
            hand_on(7)
            scores_rows(2 * pp[6] + half)
            have(('d', 6))
            scores_rows(2 * pp[6] + other)
            scores_rows(2 * pp[7] + half)
            have(('d', 7))
            scores_rows(2 * pp[7] + other)

    def sum_tiles(own, parts, cps):
        tot = own[...]
        for j, cp in zip(range(1, np_), cps):
            cp.wait_recv()
            tot = tot + parts[j]
        return tot

    def row_tile(own, parts, ss, rs_):
        return [send(own, parts.at[j], ss.at[j], rs_.at[j], j, 0) for j in range(1, np_)]

    for it in range(ITERS):
        last = it == ITERS - 1
        for i in range(8):
            ctx[it, i:i + 1] = crow[i]
        nc = 8
        if it == 1:
            nc = 16
            dfull = sum_tiles(dtx, drx, dcps)
            dscale = inv_scale / dfull
            ctx[it, 8:16] = dscale
        cps = [send(ctx.at[it, 0:nc], crx.at[it, j, 0:nc], cs.at[it, j], cr.at[it, j], 0, j) for j in range(1, nd)]
        background(it, True)
        ctot = ctx[it, 0:8]
        for j, cp in zip(range(1, nd), cps):
            cp.wait_recv()
            ctot = ctot + crx[it, j, 0:8]
        if it == 1:
            dall[d] = dscale
            for j in range(1, nd):
                dall[dp[j]] = crx[it, j, 8:16]
        vt = 1.0 / (total_protos * ctot)
        for v in range(2):
            for i in range(4):
                vrep[v, i * L:(i + 1) * L] = jnp.broadcast_to(row_to_col(eye, vt[4 * v + i:4 * v + i + 1]), (L, L))
        for v in range(2):
            racc = [jnp.zeros((8, L), F32) for _ in range(4)]
            for ck in range(B // CH):
                rows = pl.ds(ck * CH, CH)
                wv = vrep[v, rows]
                for j in range(4):
                    m = A[v, rows, j * L:(j + 1) * L] * wv
                    racc[j] = racc[j] + jnp.sum(m.reshape(CH // 8, 8, L), axis=0)
            for j in range(4):
                rtx[it, 4 * v + j:4 * v + j + 1] = jnp.sum(racc[j], axis=0, keepdims=True)
        cps = row_tile(rtx.at[it], rrx.at[it], rs.at[it], rr.at[it])
        if it == 0:
            for i in range(8):
                dtx[i:i + 1] = dsum[i]
            dcps = row_tile(dtx, drx, ts.at[0], tr.at[0])
        if last:
            vvec[p] = vt
            vcps = [send(vvec.at[p], vvec.at[p], vs.at[j], vr.at[j], j, 0) for j in range(1, np_)]
            for v in range(2):
                tacc = [jnp.zeros((8, L), F32) for _ in range(4)]
                for ck in range(B // CH):
                    rows = pl.ds(ck * CH, CH)
                    wv = vrep[v, rows]
                    for j in range(4):
                        lanes = slice(j * L, (j + 1) * L)
                        mt = A[v, rows, lanes] * wv * T[1 - v, rows, lanes]
                        tacc[j] = tacc[j] + jnp.sum(mt.reshape(CH // 8, 8, L), axis=0)
                for j in range(4):
                    ttx[4 * v + j:4 * v + j + 1] = jnp.sum(tacc[j], axis=0, keepdims=True)
            tcps = row_tile(ttx, trx, ts.at[1], tr.at[1])
        background(it, False)
        rtot = sum_tiles(rtx.at[it], rrx.at[it], cps)
        u_tile = 1.0 / (total_rows * rtot)
        if not last:
            for v in range(2):
                cols = []
                for ck in range(B // CH):
                    rows = pl.ds(ck * CH, CH)
                    part = None
                    for j in range(4):
                        m = A[v, rows, j * L:(j + 1) * L] * u_tile[4 * v + j:4 * v + j + 1]
                        part = m if part is None else part + m
                    cols.append(jnp.sum(part, axis=1, keepdims=True))
                per = L // CH
                for i in range(4):
                    crow[4 * v + i] = col_to_row(eye, jnp.concatenate(cols[per * i:per * (i + 1)], axis=0))

    w = total_rows * u_tile
    useg = w * inv_scale / (dscale * dscale)
    rowv[d, 0:8] = useg
    ucps = [send(rowv.at[d, 0:8], rowv.at[d, 0:8], us.at[0, j], ur.at[0, j], 0, j) for j in range(1, nd)]
    for i in range(8):
        ucol[i // 4, (i % 4) * L:(i % 4 + 1) * L] = jnp.broadcast_to(row_to_col(eye, useg[i:i + 1]), (L, L))
    ttot = sum_tiles(ttx, trx, tcps)
    logd = jnp.log(dfull)
    swapped = jnp.concatenate([logd[4:8], logd[0:4]], axis=0)
    terms = w * ttot * LN2 - (w * rtot) * swapped
    tot = jnp.sum(jnp.sum(terms, axis=1, keepdims=True), axis=0, keepdims=True)
    rowv[d, 8:16] = jnp.broadcast_to(tot, (8, L))
    ucps += [send(rowv.at[d, 8:16], rowv.at[d, 8:16], us.at[1, j], ur.at[1, j], 0, j) for j in range(1, nd)]
    for cp in vcps:
        cp.wait_recv()
    dz_blocks(E, vvec, ucol, H, call, G, p, np_)
    for cp in ucps:
        cp.wait_recv()
    for cp in pend:
        cp.wait_send()


def grads_kernel(np_, nd, zall, call, E, ET, rowv, vvec, vrep, ucol, G, q1, q2, loss, g1, g2, gp,
                 H, qbuf, gsum, sem):
    p = lax.axis_index('proto')
    d = lax.axis_index('data')
    total_rows = nd * B
    scale = 2 * total_rows * TEMP_TAU
    inv_scale = 1.0 / scale
    lsum = rowv[0, 8:9, 0:1]
    for k in range(1, nd):
        lsum = lsum + rowv[k, 8:9, 0:1]
    loss[...] = lsum * (-1.0 / (2 * total_rows))

    vt = vvec[p] * scale

    def codes(ck, carry):
        rows = pl.ds(pl.multiple_of(ck * CH, CH), CH)
        for v in range(2):
            uv = ucol[v, rows]
            for j in range(4):
                e = E[v, 2 * p + j // 2, rows, (j % 2) * L:(j % 2 + 1) * L]
                qbuf[v, rows, j * L:(j + 1) * L] = (e * e) * uv * vt[4 * v + j:4 * v + j + 1]
        return carry

    lax.fori_loop(0, B // CH, codes, 0)
    out = [pltpu.make_async_copy(qbuf.at[0], q1, sem.at[0]), pltpu.make_async_copy(qbuf.at[1], q2, sem.at[1])]
    for cp in out:
        cp.start()

    gout = [pltpu.make_async_copy(G.at[0], g1, sem.at[2]), pltpu.make_async_copy(G.at[1], g2, sem.at[3])]
    for cp in gout:
        cp.start()

    def form_cols(Hs, k):
        rv = rowv[k, 0:8]
        for ck in range(B // RC):
            rows = pl.ds(ck * RC, RC)
            v1, v2 = vrep[0, rows], vrep[1, rows]
            for j in range(4):
                lanes = slice((j % 2) * L, (j % 2 + 1) * L)
                p1 = ET[0, 2 * k + j // 2, rows, lanes]
                p2 = ET[1, 2 * k + j // 2, rows, lanes]
                a1 = (p1 * p1) * rv[j:j + 1] * v1
                a2 = (p2 * p2) * rv[4 + j:5 + j] * v2
                Hs[0, j, rows] = (p1 - a2).astype(BF16)
                Hs[1, j, rows] = (p2 - a1).astype(BF16)

    form_cols(H.at[0], 0)
    gsum[...] = jnp.zeros_like(gsum)

    def two(i, carry):
        for s in range(2):
            k = 2 * i + s
            t = [jnp.dot(slabs(H.at[s], v), zall[v, pl.ds(2 * k, 2)].reshape(B, -1), preferred_element_type=F32) for v in range(2)]
            gsum[...] += t[0] + t[1]
            form_cols(H.at[1 - s], lax.rem(k + 1, nd))
        return carry

    lax.fori_loop(0, nd // 2, two, 0)
    gout.append(pltpu.make_async_copy(gsum, gp, sem.at[4]))
    gout[-1].start()
    for cp in out + gout:
        cp.wait()


def solution(mesh):
    np_ = mesh.shape['proto']
    nd = mesh.shape['data']
    VM = pl.BlockSpec(memory_space=pltpu.VMEM)
    HBM = pl.BlockSpec(memory_space=pltpu.HBM)
    ANY = pl.BlockSpec(memory_space=pl.ANY)
    DMA = pltpu.SemaphoreType.DMA

    def local_step(emb_one, emb_two, protos):
        dim = protos.shape[1]
        sds = jax.ShapeDtypeStruct
        mid = pl.pallas_call(
            functools.partial(sinkhorn_kernel, np_, nd),
            out_shape=(sds((2, 2 * nd, HB, dim), BF16), sds((2 * np_, HB, dim), BF16),
                       sds((2, 2 * np_, B, HB), F32), sds((2, 2 * nd, B, HB), F32),
                       sds((nd, 16, L), F32), sds((np_, 8, L), F32),
                       sds((2, B, L), F32), sds((4, B, L), F32), sds((2, B, dim), F32)),
            in_specs=[HBM] * 3, out_specs=(VM,) * 9,
            scratch_shapes=[
                pltpu.VMEM((2, B, B), F32), pltpu.VMEM((2, B, B), F32), pltpu.VMEM((2, 2, 4, B, L), BF16),
                pltpu.VMEM((nd, 8, L), F32),
                pltpu.VMEM((ITERS, 16, L), F32), pltpu.VMEM((ITERS, nd, 16, L), F32),
                pltpu.VMEM((ITERS, 8, L), F32), pltpu.VMEM((ITERS, np_, 8, L), F32),
                pltpu.VMEM((8, L), F32), pltpu.VMEM((np_, 8, L), F32), pltpu.VMEM((8, L), F32), pltpu.VMEM((np_, 8, L), F32),
                DMA((6,)), DMA((ITERS, nd)), DMA((ITERS, nd)), DMA((ITERS, np_)), DMA((ITERS, np_)),
                DMA((np_,)), DMA((np_,)), DMA((2, nd)), DMA((2, nd)), DMA((2, np_)), DMA((2, np_)),
                DMA((12,)), DMA((12,)), DMA((15,)), DMA((15,)), DMA((np_,)), DMA((np_,))],
            compiler_params=pltpu.CompilerParams(collective_id=0, has_side_effects=True, vmem_limit_bytes=10 << 20),
            name='sinkhorn',
        )(*[pltpu.with_memory_space_constraint(a, pltpu.HBM) for a in (emb_one, emb_two, protos)])
        q1, q2, loss, g1, g2, gp = pl.pallas_call(
            functools.partial(grads_kernel, np_, nd),
            out_shape=(sds((B, B), F32), sds((B, B), F32), sds((1, 1), F32),
                       sds((B, dim), F32), sds((B, dim), F32), sds((B, dim), F32)),
            in_specs=[VM] * 9, out_specs=(ANY, ANY, VM, ANY, ANY, ANY),
            scratch_shapes=[pltpu.VMEM((2, 2, 4, B, L), BF16), pltpu.VMEM((2, B, B), F32),
                            pltpu.VMEM((B, dim), F32), DMA((5,))],
            compiler_params=pltpu.CompilerParams(vmem_limit_bytes=17 << 20),
            name='grads',
        )(*mid)
        return q1, q2, loss.reshape(()), g1, g2, gp

    return jax.shard_map(
        local_step, mesh=mesh,
        in_specs=(P('data', None), P('data', None), P('proto', None)),
        out_specs=(P('data', 'proto'), P('data', 'proto'), P(), P('data', None), P('data', None), P('proto', None)),
        check_vma=False)
```

```python
import functools
import math

import jax
import jax.numpy as jnp
from jax import lax
from jax.experimental import pallas as pl
from jax.experimental.pallas import tpu as pltpu
from jax.sharding import PartitionSpec as P

TEMP_TAU = 0.1
ITERS = 3
F32, BF16 = jnp.float32, jnp.bfloat16
LOG2E_TAU = math.log2(math.e) / TEMP_TAU
LN2 = math.log(2.0)
B = 512
HB = 256
L = 128
CH = 64
RC = 16
NT = (((1,), (1,)), ((), ()))


def eye_mask():
    return lax.broadcasted_iota(jnp.int32, (L, L), 0) == lax.broadcasted_iota(jnp.int32, (L, L), 1)


def col_to_row(eye, col):
    return jnp.sum(jnp.where(eye, col, 0.0), axis=0, keepdims=True)


def row_to_col(eye, row):
    return jnp.sum(jnp.where(eye, row, 0.0), axis=1, keepdims=True)


def xor(a, k):
    out = a
    for bit in (1, 2, 4):
        if k & bit:
            out = out + bit - 2 * bit * lax.rem(out // bit, 2)
    return out


def xor2(a, b):
    out = 0
    for bit in (1, 2, 4):
        out = out + bit * lax.rem(lax.rem(a // bit, 2) + lax.rem(b // bit, 2), 2)
    return out


def form_rows(E, vvec, ucol, H, q):
    vq = vvec[q]
    for ck in range(B // RC):
        rows = pl.ds(ck * RC, RC)
        u1, u2 = ucol[0, rows], ucol[1, rows]
        for j in range(4):
            lanes = slice((j % 2) * L, (j % 2 + 1) * L)
            p1 = E[0, 2 * q + j // 2, rows, lanes]
            p2 = E[1, 2 * q + j // 2, rows, lanes]
            a1 = (p1 * p1) * u1 * vq[j:j + 1]
            a2 = (p2 * p2) * u2 * vq[4 + j:5 + j]
            H[0, j, rows] = (p1 - a2).astype(BF16)
            H[1, j, rows] = (p2 - a1).astype(BF16)


def dz_blocks(E, vvec, ucol, H, call, G, p, n):
    form_rows(E, vvec, ucol, H.at[0], p)
    G[...] = jnp.zeros_like(G)

    def two(i, carry):
        for s in range(2):
            j = 2 * i + s
            q = xor2(p, j)
            for v in range(2):
                G[v] += times_block(H.at[s], v, call, q)
            form_rows(E, vvec, ucol, H.at[1 - s], xor2(p, lax.rem(j + 1, 8)))
        return carry

    lax.fori_loop(0, n // 2 - 1, two, 0)
    qa, qb = xor2(p, n - 2), xor2(p, n - 1)
    for v in range(2):
        G[v] += times_block(H.at[0], v, call, qa)
    form_rows(E, vvec, ucol, H.at[1], qb)
    for v in range(2):
        G[v] += times_block(H.at[1], v, call, qb)


def slabs(H, v):
    return jnp.concatenate([H[v, j] for j in range(4)], axis=1)


def times_block(H, v, call, q):
    return jnp.dot(slabs(H, v), call[pl.ds(2 * q, 2)].reshape(B, -1), preferred_element_type=F32)


def sinkhorn_kernel(np_, nd, z1, z2, c, zall, call, E, ET, rowv, vvec, vrep, ucol, G,
                    T, A, H, dall, ctx, crx, rtx, rrx, dtx, drx, ttx, trx,
                    lsem, cs, cr, rs, rr, vs, vr, us, ur, ts, tr, zs, zr, gs, gr, ds_, dr_):
    p = lax.axis_index('proto')
    d = lax.axis_index('data')
    total_rows = nd * B
    total_protos = np_ * B
    inv_scale = 1.0 / (2 * total_rows * TEMP_TAU)
    half = lax.rem(d, 2)
    other = 1 - half

    loads = [pltpu.make_async_copy(z1.at[h * HB:(h + 1) * HB], zall.at[0, 2 * d + h], lsem.at[h]) for h in range(2)]
    loads += [pltpu.make_async_copy(z2.at[h * HB:(h + 1) * HB], zall.at[1, 2 * d + h], lsem.at[2 + h]) for h in range(2)]
    loads += [pltpu.make_async_copy(c.at[h * HB:(h + 1) * HB], call.at[2 * p + h], lsem.at[4 + h]) for h in range(2)]
    for cp in loads:
        cp.start()

    dp = [xor(d, j) for j in range(nd)]
    pp = [xor(p, j) for j in range(np_)]

    bar = pltpu.get_barrier_semaphore()
    for j in range(1, nd):
        pl.semaphore_signal(bar, inc=1, device_id={'proto': p, 'data': dp[j]})
    for j in range(1, np_):
        pl.semaphore_signal(bar, inc=1, device_id={'proto': pp[j], 'data': d})

    for cp in loads:
        cp.wait()

    pend = []

    def send(src, dst, ss, rs_, pj, dj):
        cp = pltpu.make_async_remote_copy(src, dst, ss, rs_, device_id={'proto': pp[pj], 'data': dp[dj]})
        cp.start()
        pend.append(cp)
        return cp

    def z_x(i):
        ref = zall.at[i // 2, 2 * d + i % 2]
        return send(ref, ref, zs.at[i], zr.at[i], 0, 2)

    def z_partner(slot, v, nb):
        ref = zall.at[v, nb]
        return send(ref, ref, zs.at[slot], zr.at[slot], 0, 1)

    quarter = pl.ds(pl.multiple_of(d // 2 * L, L), L)

    def c_send(slot, q, pj, dj=0, whole=False):
        ref = call.at[2 * q + half] if whole else call.at[2 * q + half, quarter]
        return send(ref, ref, gs.at[slot], gr.at[slot], pj, dj)

    def c_partner(j):
        ref = call.at[2 * pp[j] + half]
        return send(ref, ref, ds_.at[j], dr_.at[j], 0, 1)

    def own_images(v):
        return zall[v, pl.ds(2 * d, 2)].reshape(B, -1)

    def own_protos():
        return call[pl.ds(2 * p, 2)].reshape(B, -1)

    def scores_rows(hb):
        for v in range(2):
            s = lax.dot_general(own_images(v), call[hb], NT, preferred_element_type=F32)
            for j in range(2):
                lanes = slice(j * L, (j + 1) * L)
                E[v, hb, :, lanes] = jnp.exp2(s[:, lanes] * LOG2E_TAU) * ucol[2 + v]

    def scores_cols(nb):
        for v in range(2):
            s = lax.dot_general(own_protos(), zall[v, nb], NT, preferred_element_type=F32)
            for j in range(2):
                lanes = slice(j * L, (j + 1) * L)
                row = pl.ds(4 * v + 2 * lax.rem(nb, 2) + j, 1)
                ET[v, nb, :, lanes] = jnp.exp2(s[:, lanes] * LOG2E_TAU) * dall[nb // 2, row]

    eye = eye_mask()

    crow = [None] * 8
    dsum = [None] * 8
    for v in range(2):
        dacc = [None] * 4
        for h in range(2):
            part = None
            for h2 in range(2):
                s = lax.dot_general(call[2 * p + h], zall[v, 2 * d + h2], NT, preferred_element_type=F32)
                e = jnp.exp2(s * LOG2E_TAU)
                A[v, h * HB:(h + 1) * HB, h2 * HB:(h2 + 1) * HB] = e
                a = e * e
                for j in range(2):
                    lanes = slice(j * L, (j + 1) * L)
                    ds = jnp.sum(e[:, lanes].reshape(HB // 8, 8, L), axis=0)
                    k = 2 * h2 + j
                    dacc[k] = ds if dacc[k] is None else dacc[k] + ds
                    part = a[:, lanes] if part is None else part + a[:, lanes]
            col = jnp.sum(part, axis=1, keepdims=True)
            for i in range(2):
                crow[4 * v + 2 * h + i] = col_to_row(eye, col[i * L:(i + 1) * L])
        for j in range(4):
            dsum[4 * v + j] = jnp.sum(dacc[j], axis=0, keepdims=True)

    pl.semaphore_wait(bar, nd - 1 + np_ - 1)

    bulk = {}

    def c_x(j):
        bulk['x', j] = c_send(7 + j, pp[j], 0, 2)

    def have(*keys):
        for key in keys:
            bulk[key].wait_recv()

    def hand_on(j):
        bulk['d', j] = c_partner(j)

    def background(it, along_data):
        if it == 0 and along_data:
            bulk['y', 0] = c_send(0, p, 1, whole=True)
            bulk['z', 2] = c_send(1, p, 2)
            bulk['z', 4] = c_send(2, p, 4)
            bulk['zx', 0] = z_x(0)
            for i in range(4):
                bulk['zp', i] = z_partner(4 + i, i // 2, 2 * d + i % 2)
            for v in range(2):
                for ck in range(B // CH):
                    rows = pl.ds(ck * CH, CH)
                    e = A[v, rows]
                    for h in range(2):
                        ET[v, 2 * d + h, rows] = e[:, h * HB:(h + 1) * HB]
                    A[v, rows] = e * e
            for v in range(2):
                T[v] = lax.dot_general(own_protos(), own_images(v), NT, preferred_element_type=F32) * LOG2E_TAU
        elif it == 0:
            bulk['zx', 1] = z_x(1)
            have(('z', 2))
            c_x(2)
            bulk['y', 2] = c_send(4, pp[2], 1)
            have(('y', 0))
            hand_on(1)
            have(('z', 4))
            bulk['y', 4] = c_send(5, pp[4], 1)
        elif it == 1 and along_data:
            bulk['z', 6] = c_send(3, p, 6)
            c_x(4)
            have(('y', 2))
            c_x(3)
            bulk['zx', 2] = z_x(2)
            have(('y', 4))
            c_x(5)
            for i in range(8):
                ucol[2 + i // 4, (i % 4) * L:(i % 4 + 1) * L] = jnp.broadcast_to(
                    row_to_col(eye, dscale[i:i + 1]), (L, L))
            scores_rows(2 * p)
            scores_rows(2 * p + 1)
            have(('x', 2))
            hand_on(2)
            scores_rows(2 * pp[1] + half)
        elif it == 1:
            have(('x', 4))
            hand_on(4)
            have(('d', 1))
            scores_rows(2 * pp[1] + other)
            scores_rows(2 * pp[2] + half)
            have(('d', 2))
            scores_rows(2 * pp[2] + other)
            have(('z', 6))
            c_x(6)
            bulk['y', 6] = c_send(6, pp[6], 1)
            have(('zp', 0), ('zp', 1), ('zp', 2), ('zp', 3))
            scores_cols(2 * dp[1])
            scores_cols(2 * dp[1] + 1)
            for v in range(2):
                for h in range(2):
                    for j in range(2):
                        lanes = slice(j * L, (j + 1) * L)
                        k = 4 * v + 2 * h + j
                        ET[v, 2 * d + h, :, lanes] = ET[v, 2 * d + h, :, lanes] * dscale[k:k + 1]
            scores_rows(2 * pp[4] + half)
        elif it == 2 and along_data:
            bulk['zx', 3] = z_x(3)
            have(('x', 3))
            hand_on(3)
            have(('x', 5))
            hand_on(5)
            have(('d', 4))
            scores_rows(2 * pp[4] + other)
            for i in range(3):
                have(('zx', i))
                bulk['zf', i] = z_partner(8 + i, i // 2, 2 * dp[2] + i % 2)
            scores_rows(2 * pp[3] + half)
            scores_rows(2 * pp[5] + half)
        elif it == 2:
            have(('y', 6))
            c_x(7)
            have(('x', 6))
            hand_on(6)
            have(('zx', 3))
            bulk['zf', 3] = z_partner(11, 1, 2 * dp[2] + 1)
            for j in (3, 5):
                have(('d', j))
                scores_rows(2 * pp[j] + other)
            scores_cols(2 * dp[2])
            scores_cols(2 * dp[2] + 1)
            have(('zf', 0), ('zf', 1), ('zf', 2), ('zf', 3))
            scores_cols(2 * dp[3])
            scores_cols(2 * dp[3] + 1)
            have(('x', 7))
            hand_on(7)
            scores_rows(2 * pp[6] + half)
            have(('d', 6))
            scores_rows(2 * pp[6] + other)
            scores_rows(2 * pp[7] + half)
            have(('d', 7))
            scores_rows(2 * pp[7] + other)

    def sum_tiles(own, parts, cps):
        tot = own[...]
        for j, cp in zip(range(1, np_), cps):
            cp.wait_recv()
            tot = tot + parts[j]
        return tot

    def row_tile(own, parts, ss, rs_):
        return [send(own, parts.at[j], ss.at[j], rs_.at[j], j, 0) for j in range(1, np_)]

    for it in range(ITERS):
        last = it == ITERS - 1
        for i in range(8):
            ctx[it, i:i + 1] = crow[i]
        nc = 8
        if it == 1:
            nc = 16
            dfull = sum_tiles(dtx, drx, dcps)
            dscale = inv_scale / dfull
            ctx[it, 8:16] = dscale
        cps = [send(ctx.at[it, 0:nc], crx.at[it, j, 0:nc], cs.at[it, j], cr.at[it, j], 0, j) for j in range(1, nd)]
        background(it, True)
        ctot = ctx[it, 0:8]
        for j, cp in zip(range(1, nd), cps):
            cp.wait_recv()
            ctot = ctot + crx[it, j, 0:8]
        if it == 1:
            dall[d] = dscale
            for j in range(1, nd):
                dall[dp[j]] = crx[it, j, 8:16]
        vt = 1.0 / (total_protos * ctot)
        for v in range(2):
            for i in range(4):
                vrep[v, i * L:(i + 1) * L] = jnp.broadcast_to(row_to_col(eye, vt[4 * v + i:4 * v + i + 1]), (L, L))
        for v in range(2):
            racc = [jnp.zeros((8, L), F32) for _ in range(4)]
            for ck in range(B // CH):
                rows = pl.ds(ck * CH, CH)
                wv = vrep[v, rows]
                for j in range(4):
                    m = A[v, rows, j * L:(j + 1) * L] * wv
                    racc[j] = racc[j] + jnp.sum(m.reshape(CH // 8, 8, L), axis=0)
            for j in range(4):
                rtx[it, 4 * v + j:4 * v + j + 1] = jnp.sum(racc[j], axis=0, keepdims=True)
        cps = row_tile(rtx.at[it], rrx.at[it], rs.at[it], rr.at[it])
        if it == 0:
            for i in range(8):
                dtx[i:i + 1] = dsum[i]
            dcps = row_tile(dtx, drx, ts.at[0], tr.at[0])
        if last:
            vvec[p] = vt
            vcps = [send(vvec.at[p], vvec.at[p], vs.at[j], vr.at[j], j, 0) for j in range(1, np_)]
            for v in range(2):
                tacc = [jnp.zeros((8, L), F32) for _ in range(4)]
                for ck in range(B // CH):
                    rows = pl.ds(ck * CH, CH)
                    wv = vrep[v, rows]
                    for j in range(4):
                        lanes = slice(j * L, (j + 1) * L)
                        mt = A[v, rows, lanes] * wv * T[1 - v, rows, lanes]
                        tacc[j] = tacc[j] + jnp.sum(mt.reshape(CH // 8, 8, L), axis=0)
                for j in range(4):
                    ttx[4 * v + j:4 * v + j + 1] = jnp.sum(tacc[j], axis=0, keepdims=True)
            tcps = row_tile(ttx, trx, ts.at[1], tr.at[1])
        background(it, False)
        rtot = sum_tiles(rtx.at[it], rrx.at[it], cps)
        u_tile = 1.0 / (total_rows * rtot)
        if not last:
            for v in range(2):
                cols = []
                for ck in range(B // CH):
                    rows = pl.ds(ck * CH, CH)
                    part = None
                    for j in range(4):
                        m = A[v, rows, j * L:(j + 1) * L] * u_tile[4 * v + j:4 * v + j + 1]
                        part = m if part is None else part + m
                    cols.append(jnp.sum(part, axis=1, keepdims=True))
                per = L // CH
                for i in range(4):
                    crow[4 * v + i] = col_to_row(eye, jnp.concatenate(cols[per * i:per * (i + 1)], axis=0))

    w = total_rows * u_tile
    useg = w * inv_scale / (dscale * dscale)
    rowv[d, 0:8] = useg
    ucps = [send(rowv.at[d, 0:8], rowv.at[d, 0:8], us.at[0, j], ur.at[0, j], 0, j) for j in range(1, nd)]
    for i in range(8):
        ucol[i // 4, (i % 4) * L:(i % 4 + 1) * L] = jnp.broadcast_to(row_to_col(eye, useg[i:i + 1]), (L, L))
    ttot = sum_tiles(ttx, trx, tcps)
    logd = jnp.log(dfull)
    swapped = jnp.concatenate([logd[4:8], logd[0:4]], axis=0)
    terms = w * ttot * LN2 - (w * rtot) * swapped
    tot = jnp.sum(jnp.sum(terms, axis=1, keepdims=True), axis=0, keepdims=True)
    rowv[d, 8:16] = jnp.broadcast_to(tot, (8, L))
    ucps += [send(rowv.at[d, 8:16], rowv.at[d, 8:16], us.at[1, j], ur.at[1, j], 0, j) for j in range(1, nd)]
    for cp in vcps:
        cp.wait_recv()
    dz_blocks(E, vvec, ucol, H, call, G, p, np_)
    for cp in ucps:
        cp.wait_recv()
    for cp in pend:
        cp.wait_send()


def grads_kernel(np_, nd, zall, call, E, ET, rowv, vvec, vrep, ucol, G, q1, q2, loss, g1, g2, gp,
                 H, qbuf, gsum, sem):
    p = lax.axis_index('proto')
    d = lax.axis_index('data')
    total_rows = nd * B
    scale = 2 * total_rows * TEMP_TAU
    inv_scale = 1.0 / scale
    lsum = rowv[0, 8:9, 0:1]
    for k in range(1, nd):
        lsum = lsum + rowv[k, 8:9, 0:1]
    loss[...] = lsum * (-1.0 / (2 * total_rows))

    vt = vvec[p] * scale

    def codes(ck, carry):
        rows = pl.ds(pl.multiple_of(ck * CH, CH), CH)
        for v in range(2):
            uv = ucol[v, rows]
            for j in range(4):
                e = E[v, 2 * p + j // 2, rows, (j % 2) * L:(j % 2 + 1) * L]
                qbuf[v, rows, j * L:(j + 1) * L] = (e * e) * uv * vt[4 * v + j:4 * v + j + 1]
        return carry

    lax.fori_loop(0, B // CH, codes, 0)
    out = [pltpu.make_async_copy(qbuf.at[0], q1, sem.at[0]), pltpu.make_async_copy(qbuf.at[1], q2, sem.at[1])]
    for cp in out:
        cp.start()

    gout = [pltpu.make_async_copy(G.at[0], g1, sem.at[2]), pltpu.make_async_copy(G.at[1], g2, sem.at[3])]
    for cp in gout:
        cp.start()

    def form_cols(Hs, k):
        rv = rowv[k, 0:8]
        for ck in range(B // RC):
            rows = pl.ds(ck * RC, RC)
            v1, v2 = vrep[0, rows], vrep[1, rows]
            for j in range(4):
                lanes = slice((j % 2) * L, (j % 2 + 1) * L)
                p1 = ET[0, 2 * k + j // 2, rows, lanes]
                p2 = ET[1, 2 * k + j // 2, rows, lanes]
                a1 = (p1 * p1) * rv[j:j + 1] * v1
                a2 = (p2 * p2) * rv[4 + j:5 + j] * v2
                Hs[0, j, rows] = (p1 - a2).astype(BF16)
                Hs[1, j, rows] = (p2 - a1).astype(BF16)

    form_cols(H.at[0], 0)
    gsum[...] = jnp.zeros_like(gsum)

    def two(i, carry):
        for s in range(2):
            k = 2 * i + s
            t = [jnp.dot(slabs(H.at[s], v), zall[v, pl.ds(2 * k, 2)].reshape(B, -1), preferred_element_type=F32) for v in range(2)]
            gsum[...] += t[0] + t[1]
            form_cols(H.at[1 - s], lax.rem(k + 1, nd))
        return carry

    lax.fori_loop(0, nd // 2 - 1, two, 0)
    for s, k in ((0, nd - 2), (1, nd - 1)):
        t = [jnp.dot(slabs(H.at[s], v), zall[v, 2 * k:2 * k + 2].reshape(B, -1), preferred_element_type=F32) for v in range(2)]
        gsum[...] += t[0] + t[1]
        if s == 0:
            form_cols(H.at[1], nd - 1)
    gout.append(pltpu.make_async_copy(gsum, gp, sem.at[4]))
    gout[-1].start()
    for cp in out + gout:
        cp.wait()


def solution(mesh):
    np_ = mesh.shape['proto']
    nd = mesh.shape['data']
    VM = pl.BlockSpec(memory_space=pltpu.VMEM)
    HBM = pl.BlockSpec(memory_space=pltpu.HBM)
    ANY = pl.BlockSpec(memory_space=pl.ANY)
    DMA = pltpu.SemaphoreType.DMA

    def local_step(emb_one, emb_two, protos):
        dim = protos.shape[1]
        sds = jax.ShapeDtypeStruct
        mid = pl.pallas_call(
            functools.partial(sinkhorn_kernel, np_, nd),
            out_shape=(sds((2, 2 * nd, HB, dim), BF16), sds((2 * np_, HB, dim), BF16),
                       sds((2, 2 * np_, B, HB), F32), sds((2, 2 * nd, B, HB), F32),
                       sds((nd, 16, L), F32), sds((np_, 8, L), F32),
                       sds((2, B, L), F32), sds((4, B, L), F32), sds((2, B, dim), F32)),
            in_specs=[HBM] * 3, out_specs=(VM,) * 9,
            scratch_shapes=[
                pltpu.VMEM((2, B, B), F32), pltpu.VMEM((2, B, B), F32), pltpu.VMEM((2, 2, 4, B, L), BF16),
                pltpu.VMEM((nd, 8, L), F32),
                pltpu.VMEM((ITERS, 16, L), F32), pltpu.VMEM((ITERS, nd, 16, L), F32),
                pltpu.VMEM((ITERS, 8, L), F32), pltpu.VMEM((ITERS, np_, 8, L), F32),
                pltpu.VMEM((8, L), F32), pltpu.VMEM((np_, 8, L), F32), pltpu.VMEM((8, L), F32), pltpu.VMEM((np_, 8, L), F32),
                DMA((6,)), DMA((ITERS, nd)), DMA((ITERS, nd)), DMA((ITERS, np_)), DMA((ITERS, np_)),
                DMA((np_,)), DMA((np_,)), DMA((2, nd)), DMA((2, nd)), DMA((2, np_)), DMA((2, np_)),
                DMA((12,)), DMA((12,)), DMA((15,)), DMA((15,)), DMA((np_,)), DMA((np_,))],
            compiler_params=pltpu.CompilerParams(collective_id=0, has_side_effects=True, vmem_limit_bytes=10 << 20),
            name='sinkhorn',
        )(*[pltpu.with_memory_space_constraint(a, pltpu.HBM) for a in (emb_one, emb_two, protos)])
        q1, q2, loss, g1, g2, gp = pl.pallas_call(
            functools.partial(grads_kernel, np_, nd),
            out_shape=(sds((B, B), F32), sds((B, B), F32), sds((1, 1), F32),
                       sds((B, dim), F32), sds((B, dim), F32), sds((B, dim), F32)),
            in_specs=[VM] * 9, out_specs=(ANY, ANY, VM, ANY, ANY, ANY),
            scratch_shapes=[pltpu.VMEM((2, 2, 4, B, L), BF16), pltpu.VMEM((2, B, B), F32),
                            pltpu.VMEM((B, dim), F32), DMA((5,))],
            compiler_params=pltpu.CompilerParams(vmem_limit_bytes=17 << 20),
            name='grads',
        )(*mid)
        return q1, q2, loss.reshape(()), g1, g2, gp

    return jax.shard_map(
        local_step, mesh=mesh,
        in_specs=(P('data', None), P('data', None), P('proto', None)),
        out_specs=(P('data', 'proto'), P('data', 'proto'), P(), P('data', None), P('data', None), P('proto', None)),
        check_vma=False)
```
